512 devices in a mesh: panel: 128 (over z, y, core), obs: 4 (over x).
Axes of the slice: x: 4, y: 4, z: 16, core: 2. Of those that a mesh axis runs over, the one named last changes fastest.
Arguments:
- flow_blocks: bfloat16 [16384, 4, 1280], P('panel'), may hold values from -6 to 6
- interp_weights: bfloat16 [512, 128, 512], P(('panel', 'obs')), may hold values from -0.25 to 0.25
- donor_owner: int32 [65536, 1], P(('panel', 'obs')), may hold values from 0 to 127; in each aligned block of 128 rows (0 to 127, 128 to 255, ...) at most 2 rows name the same one
- donor_block: int32 [65536], P(('panel', 'obs')), may hold values from 0 to 127
- panel_normals: float32 [3, 65536], P(None, ('panel', 'obs')), may hold values from -0.75 to 0.75
- panel_points: float32 [3, 65536], P(None, ('panel', 'obs')), may hold values from -1 to 1
- observer_points: float32 [3, 1024], P(None, 'obs'), may hold values from -12 to 12, as said below
Outputs:
- pressure: float32 [128, 1024], P('panel', 'obs')
The draws below stay inside these ranges and needn't reach their ends.
Inputs may be any that keep to these rules, and one draw needn't show every extreme that they name: `donor_owner`: within the rows of one device, no owner index is named by more than 2 rows; some devices' rows name one owner exactly 2 times. `observer_points`: every observer lies between 6 and 12 from the anchor.
All inputs are finite; a program needn't handle non-finite values.
Results may differ from the reference program's by a relative error of at most 0.0003.
Values may be sent and summed in bfloat16 or wider, within the bound.
No kernel may reach another device: no remote copies, remote signals or barrier semaphores. Data moves between devices by JAX's collectives and lax.ppermute only.
A program may use at most 64 MiB of HBM per device.

```python
import math
import jax
import jax.numpy as jnp
import numpy as np
from jax import lax

NV = 5
NT = 256
HARM = 64
TILE = 128
SLOTS = 128
CB = 4
GB_DEV = 128
TILE_DEV = 1
TILES = 512
PANELS = 65536
BLOCKS = 16384
OBS = 1024
CAP = 2
N_PANEL = 128


def draw_observer_points(key, part):
    key_height, key_turn, key_radius = jax.random.split(key, 3)
    height = jax.random.uniform(key_height, (OBS,), jnp.float32, -1.0, 1.0)
    turn = jax.random.uniform(key_turn, (OBS,), jnp.float32, -math.pi, math.pi)
    radius = jax.random.uniform(key_radius, (OBS,), jnp.float32, 6.0, 12.0)
    side = jnp.sqrt(jnp.maximum(1.0 - height * height, 0.0))
    return jnp.stack([radius * side * jnp.cos(turn), radius * side * jnp.sin(turn), radius * height])


def plant(array, key, smallest, top_value):
    shape = array.shape
    spot = [jax.random.randint(jax.random.fold_in(key, axis), (), 0, shape[axis]) for axis in range(len(shape))]
    array = array.at[tuple(spot)].set(smallest)
    longest = shape.index(max(shape))
    spot[longest] = (spot[longest] + 1) % shape[longest]
    return array.at[tuple(spot)].set(top_value)


def level_of(stream_key, dims, cuts, least, high):
    gain = 1.0
    for axis_at, shards_of in cuts:
        heights = jax.random.uniform(jax.random.fold_in(jax.random.fold_in(stream_key, 6), axis_at), (shards_of,), jnp.float32, least / len(cuts), high / len(cuts))
        gain = gain * jnp.repeat(jnp.exp(heights), dims[axis_at] // shards_of).reshape((-1,) + (1,) * (len(dims) - 1 - axis_at))
    return gain


def assign_block(stream_key, own, number, rows, amount, top, limit, slope):
    sequence = jax.random.permutation(stream_key, amount)
    packed, ordinary = shares(amount, rows * top, limit, slope, True), shares(amount, rows * top, limit, slope, False)
    places = jnp.arange(amount)

    def named(tallies, turn):
        used = int((tallies > 0).sum())
        fixed = max(1, used // 4)
        moved = fixed + (places - fixed + turn * (used - fixed)) % max(1, amount - fixed)
        return jnp.zeros((amount,), jnp.int32).at[sequence[jnp.where(places < fixed, places, moved)]].set(jnp.asarray(tallies, jnp.int32))

    tallies = jnp.where(number % 4 == 0, named(packed, number // 4), named(ordinary, number - number // 4 - 1))
    mixed = jax.random.permutation(jax.random.fold_in(own, 3), amount)
    donor, sink = mixed[0:amount // 2 * 2:2], mixed[1:amount // 2 * 2:2]
    slack = jnp.minimum(tallies[donor] - 1, limit - tallies[sink]) // 2
    slack = jnp.where((donor == sequence[0]) | (sink == sequence[0]) | (tallies[sink] == 0), 0, jnp.maximum(slack, 0))
    moved = jax.random.randint(jax.random.fold_in(own, 4), (amount // 2,), 0, 1 << 20) % (slack + 1)
    tallies = tallies.at[donor].add(-moved).at[sink].add(moved)
    items = jnp.searchsorted(jnp.cumsum(tallies), jnp.arange(rows * top), side="right").astype(jnp.int32)
    table = items.reshape(top, rows).T
    table = table[jax.random.permutation(jax.random.fold_in(own, 1), rows)]
    turn = jax.random.randint(jax.random.fold_in(own, 2), (rows, 1), 0, top)
    return jnp.take_along_axis(table, (jnp.arange(top)[None, :] + turn) % top, axis=1)


def shares(number_of, total, most, lean, full):
    weights = [(1 << 20) // math.isqrt(standing ** lean) + 1 for standing in range(1, number_of + 1)]
    largest = most if full else min(most, max(-(-total // number_of), total * weights[0] // sum(weights)))
    least = 1 if total - largest >= number_of - 1 else 0
    holding, surplus = [largest] + [least] * (number_of - 1), total - largest - least * (number_of - 1)
    while surplus > 0:
        candidates = [i for i in range(1, number_of) if holding[i] < largest] or [i for i in range(1, number_of) if holding[i] < most]
        whole, left = sum([weights[i] for i in candidates]), surplus
        for i in candidates:
            addition = min(most - holding[i], max(1, left * weights[i] // whole), surplus)
            holding[i] = holding[i] + addition
            surplus = surplus - addition
    return np.array(holding)


def noise(stream_key, shape, width, limit, pieces=(), kind=jnp.bfloat16):
    entries = jax.random.normal(stream_key, shape, jnp.float32) * width
    if len(pieces) > 0:
        entries = level_of(stream_key, shape, pieces, -0.22, 0.18) * entries
    return jnp.clip(entries, min=-limit, max=limit).astype(kind)


def setup_inputs(seed: int = 0) -> dict:
    arg_keys = jax.random.split(jax.random.key(seed), 8)
    flow_blocks = noise(arg_keys[0], (BLOCKS, CB, NV * NT), 1.0, 6.0, ((0, 128),))
    interp_weights = noise(arg_keys[1], (TILES, TILE, SLOTS * CB), (SLOTS * CB) ** -0.5, 0.25, ((0, 512),))
    donor_owner_keys = jax.random.split(jax.random.fold_in(arg_keys[2], 1), (TILES * SLOTS) // (TILE_DEV * SLOTS))
    donor_owner_turns = jax.random.permutation(jax.random.fold_in(arg_keys[2], 3), (TILES * SLOTS) // (TILE_DEV * SLOTS))
    donor_owner = jax.vmap(lambda own, number: assign_block(jax.random.fold_in(arg_keys[2], 2), own, number, TILE_DEV * SLOTS, N_PANEL, 1, CAP, 2))(donor_owner_keys, donor_owner_turns).reshape((TILES * SLOTS, 1))
    donor_block = plant(jax.random.randint(arg_keys[3], (TILES * SLOTS,), 0, GB_DEV), jax.random.fold_in(arg_keys[3], 1), 0, GB_DEV - 1).astype(jnp.int32)
    panel_normals = noise(arg_keys[4], (3, PANELS), (30.0 * PANELS ** -0.5), 0.75, ((1, 512),), jnp.float32)
    panel_points = jnp.clip(jax.random.uniform(arg_keys[5], (3, PANELS), jnp.float32, -1.0, 1.0) * level_of(arg_keys[5], (3, PANELS), ((1, 512),), -0.4, 0.0), -1.0, 1.0)
    observer_points = draw_observer_points(jax.random.fold_in(arg_keys[7], 71), 0)
    return dict(flow_blocks=flow_blocks, interp_weights=interp_weights, donor_owner=donor_owner, donor_block=donor_block, panel_normals=panel_normals, panel_points=panel_points, observer_points=observer_points)


KAPPA = 0.5

def fourier_table(samples, orders):
    sample_ids = jnp.arange(samples, dtype=jnp.int32)
    harmonic = jnp.arange(1, orders + 1, dtype=jnp.int32)
    wrapped = sample_ids[:, None] * harmonic[None, :] % samples
    angles = wrapped.astype(jnp.float32) * (2.0 * math.pi / samples)
    factor = 2.0 / samples
    return jnp.concatenate([factor * jnp.cos(angles), -factor * jnp.sin(angles)], axis=1)

def spectra_of(values, normals, transform, samples):
    panels = values.shape[0]
    fields = values.reshape(panels, NV, samples)
    density = 1.0 + fields[:, 0]
    velocity = fields[:, 1:4]
    pressure_pert = fields[:, 4]
    normal_vec = jnp.transpose(normals)[:, :, None]
    normal_flow = lax.optimization_barrier(jnp.sum(velocity * normal_vec, axis=1))
    mass_flux = density * normal_flow
    loading = pressure_pert[:, None, :] * normal_vec + mass_flux[:, None, :] * velocity
    series = jnp.concatenate([mass_flux[:, None, :], loading], axis=1)
    return jnp.einsum('pct,tk->ckp', series, transform, precision=lax.Precision.HIGHEST)

def radiate(spectra, points, observers):
    orders = spectra.shape[1] // 2
    offset_vec = observers[:, None, :] - points[:, :, None]
    distance = jnp.sqrt(lax.optimization_barrier(jnp.sum(offset_vec * offset_vec, axis=0)))
    inverse = 1.0 / distance
    direction = offset_vec * inverse[None]
    wavenum = (KAPPA * jnp.arange(1, orders + 1, dtype=jnp.float32))[:, None, None]
    load_re = spectra[1, :orders][:, :, None] * direction[0][None] + spectra[2, :orders][:, :, None] * direction[1][None] + spectra[3, :orders][:, :, None] * direction[2][None]
    load_im = spectra[1, orders:][:, :, None] * direction[0][None] + spectra[2, orders:][:, :, None] * direction[1][None] + spectra[3, orders:][:, :, None] * direction[2][None]
    amp_re = load_re * inverse[None] - wavenum * (spectra[0, orders:][:, :, None] + load_im)
    amp_im = load_im * inverse[None] + wavenum * (spectra[0, :orders][:, :, None] + load_re)
    phase = wavenum * distance[None]
    cosines = jnp.cos(phase)
    sines = jnp.sin(phase)
    spreading = (inverse / (4.0 * math.pi))[None]
    real_part = lax.optimization_barrier(jnp.sum((amp_re * cosines + amp_im * sines) * spreading, axis=1))
    imag_part = lax.optimization_barrier(jnp.sum((amp_im * cosines - amp_re * sines) * spreading, axis=1))
    return jnp.concatenate([real_part, imag_part], axis=0)

def reference(flow_blocks, interp_weights, donor_owner, donor_block, panel_normals, panel_points, observer_points):
    transform = fourier_table(NT, HARM)
    global_block = (donor_owner[:, 0] * GB_DEV + donor_block).astype(jnp.int32).reshape(TILES, SLOTS)
    normals_tiled = panel_normals.reshape(3, TILES, TILE).transpose(1, 0, 2)
    points_tiled = panel_points.reshape(3, TILES, TILE).transpose(1, 0, 2)

    def one_tile(running, tile_data):
        block_ids, weight_tile, normal_tile, point_tile = tile_data
        donors = flow_blocks[block_ids].reshape(SLOTS * CB, NV * NT)
        values = jnp.dot(weight_tile, donors, preferred_element_type=jnp.float32)
        spectra = spectra_of(values, normal_tile, transform, NT)
        return (running + radiate(spectra, point_tile, observer_points), None)
    initial = jnp.zeros((2 * HARM, OBS), jnp.float32)
    running, _ = lax.scan(one_tile, initial, (global_block, interp_weights, normals_tiled, points_tiled))
    return running
```

```python
import functools
import math

import jax
import jax.numpy as jnp
from jax import lax
from jax.experimental import pallas as pl
from jax.experimental.pallas import tpu as pltpu
from jax.sharding import Mesh
from jax.sharding import PartitionSpec as P

NV = 5
NT = 256
HARM = 64
KAPPA = 0.5
PANEL = ("z", "y", "c")
SLAB = ("y", "c", "x")
CAP = 2
GROUP = 8
PANEL_STEP = 8
OBS_TILE = 256


def fourier_table(samples, orders):
    sample_ids = jnp.arange(samples, dtype=jnp.int32)
    harmonic = jnp.arange(1, orders + 1, dtype=jnp.int32)
    wrapped = sample_ids[:, None] * harmonic[None, :] % samples
    angles = wrapped.astype(jnp.float32) * (2.0 * math.pi / samples)
    factor = 2.0 / samples
    return jnp.concatenate([factor * jnp.cos(angles), -factor * jnp.sin(angles)], axis=1)


def geometry_kernel(points_ref, observers_ref, basis_ref, cos_ref, sin_ref):
    panels = points_ref.shape[0]
    offsets = [observers_ref[i : i + 1, :] - points_ref[:, i : i + 1] for i in range(3)]
    distance = jnp.sqrt(offsets[0] * offsets[0] + offsets[1] * offsets[1] + offsets[2] * offsets[2])
    inverse = 1.0 / distance
    weight = inverse * (1.0 / (4.0 * math.pi))
    near = weight * inverse
    rows = lambda j: pl.ds(j, panels, stride=GROUP)
    for i in range(3):
        direction = offsets[i] * inverse
        basis_ref[rows(i), :] = direction * near
        basis_ref[rows(3 + i), :] = direction * weight
    basis_ref[rows(6), :] = weight
    basis_ref[rows(7), :] = jnp.zeros_like(weight)
    phase = KAPPA * distance
    c1, s1 = jnp.cos(phase), jnp.sin(phase)
    c, s = [c1], [s1]
    for m in range(2, GROUP + 1):
        a, b = (m // 2, m - m // 2)
        ca, sa, cb, sb = c[a - 1], s[a - 1], c[b - 1], s[b - 1]
        c.append(ca * cb - sa * sb)
        s.append(sa * cb + ca * sb)
    for m in range(GROUP):
        cos_ref[rows(m), :] = c[m]
        sin_ref[rows(m), :] = s[m]


def geometry(points, observers):
    panels, total = points.shape[0], observers.shape[1]
    tile = 128
    shape = jax.ShapeDtypeStruct((panels * GROUP, total), jnp.float32)
    spec = pl.BlockSpec((panels * GROUP, tile), lambda x: (0, x))
    return pl.pallas_call(
        geometry_kernel,
        grid=(total // tile,),
        out_shape=(shape, shape, shape),
        in_specs=[
            pl.BlockSpec((panels, 3), lambda x: (0, 0)),
            pl.BlockSpec((3, tile), lambda x: (0, x)),
        ],
        out_specs=(spec, spec, spec),
        cost_estimate=pl.CostEstimate(
            flops=200 * panels * total, bytes_accessed=12 * panels * GROUP * total, transcendentals=3 * panels * total
        ),
        name="geometry",
    )(points, observers)


def split_two(value):
    high = value.astype(jnp.bfloat16).astype(jnp.float32)
    return high, value - high


def fill_factors(values_ref, normals_ref, table_ref, factors_ref):
    panels = values_ref.shape[0]
    field = lambda v: values_ref[:, v * NT : (v + 1) * NT]
    normal = [normals_ref[:, i : i + 1] for i in range(3)]
    flow = field(1) * normal[0] + field(2) * normal[1] + field(3) * normal[2]
    mass = (1.0 + field(0)) * flow
    loads = [field(4) * normal[i] + mass * field(1 + i) for i in range(3)]
    series = jnp.concatenate([mass] + loads, axis=0)
    spectra = jnp.dot(series, table_ref[...], precision=lax.Precision.HIGHEST, preferred_element_type=jnp.float32)
    lane = lax.broadcasted_iota(jnp.int32, (panels, 2 * HARM), 1)
    order = (jnp.where(lane < HARM, lane, lane - HARM) + 1).astype(jnp.float32) * KAPPA
    wave = jnp.where(lane < HARM, -order, order)
    rows = lambda j: pl.ds(j, panels, stride=GROUP)
    for i in range(4):
        part = spectra[i * panels : (i + 1) * panels]
        turned = jnp.concatenate([part[:, HARM:], part[:, :HARM]], axis=1) * wave
        if i == 0:
            factors_ref[rows(6), :] = turned
        else:
            factors_ref[rows(i - 1), :] = part
            factors_ref[rows(2 + i), :] = turned
    factors_ref[rows(7), :] = jnp.zeros((panels, 2 * HARM), jnp.float32)


def radiate_kernel(values_ref, normals_ref, table_ref, basis_ref, cos_ref, sin_ref, out_ref, factors_ref):
    step = pl.program_id(0)

    @pl.when(step == 0)
    def _():
        fill_factors(values_ref, normals_ref, table_ref, factors_ref)
        out_ref[...] = jnp.zeros_like(out_ref)

    observers = out_ref.shape[1]
    together = 2

    def some_panels(turn, carry):
        local = [pl.multiple_of((turn * together + k) * GROUP, GROUP) for k in range(together)]
        lefts, rights = [], []
        for k in range(together):
            at = pl.multiple_of(step * (PANEL_STEP * GROUP) + local[k], GROUP)
            high, low = split_two(factors_ref[pl.ds(at, GROUP), :])
            lefts.append(jnp.concatenate([high, high, low, jnp.zeros_like(low)], axis=0).astype(jnp.bfloat16))
        for x in range(observers // OBS_TILE):
            lanes = slice(x * OBS_TILE, (x + 1) * OBS_TILE)
            amps, states = [], []
            for k in range(together):
                high, low = split_two(basis_ref[pl.ds(local[k], GROUP), lanes])
                right = jnp.concatenate([high, low, high, jnp.zeros_like(low)], axis=0).astype(jnp.bfloat16)
                amps.append(
                    lax.dot_general(lefts[k], right, (((0,), (0,)), ((), ())), preferred_element_type=jnp.float32)
                )
                c = cos_ref[pl.ds(local[k], GROUP), lanes]
                s = sin_ref[pl.ds(local[k], GROUP), lanes]
                c8 = jnp.broadcast_to(c[GROUP - 1 : GROUP, :], c.shape)
                s8 = jnp.broadcast_to(s[GROUP - 1 : GROUP, :], s.shape)
                states.append((c, s, c * c8 + s * s8, s * c8 - c * s8, 2.0 * c8))
            for g in range(HARM // GROUP):
                re = slice(g * GROUP, (g + 1) * GROUP)
                im = slice(HARM + g * GROUP, HARM + (g + 1) * GROUP)
                total_re, total_im = out_ref[re, lanes], out_ref[im, lanes]
                for k in range(together):
                    c, s, before_c, before_s, twice = states[k]
                    a_re, a_im = amps[k][re, :], amps[k][im, :]
                    total_re = total_re + (a_re * c + a_im * s)
                    total_im = total_im + (a_im * c - a_re * s)
                    states[k] = (twice * c - before_c, twice * s - before_s, c, s, twice)
                out_ref[re, lanes] = total_re
                out_ref[im, lanes] = total_im
        return carry

    lax.fori_loop(0, PANEL_STEP // together, some_panels, 0)


def radiate(values, normals, table, basis, cosines, sines):
    panels, observers = values.shape[0], basis.shape[1]
    whole = lambda a: pl.BlockSpec(a.shape, lambda p: (0,) * a.ndim)
    rows = pl.BlockSpec((PANEL_STEP * GROUP, observers), lambda p: (p, 0))
    return pl.pallas_call(
        radiate_kernel,
        grid=(panels // PANEL_STEP,),
        out_shape=jax.ShapeDtypeStruct((2 * HARM, observers), jnp.float32),
        in_specs=[whole(values), whole(normals), whole(table), rows, rows, rows],
        out_specs=pl.BlockSpec((2 * HARM, observers), lambda p: (0, 0)),
        scratch_shapes=[pltpu.VMEM((panels * GROUP, 2 * HARM), jnp.float32)],
        cost_estimate=pl.CostEstimate(
            flops=30 * panels * HARM * observers, bytes_accessed=12 * panels * GROUP * observers, transcendentals=0
        ),
        name="radiate",
    )(values, normals, table, basis, cosines, sines)


def body(flow_blocks, interp_weights, donor_owner, donor_block, panel_normals, panel_points, observer_points):
    peers = lax.axis_size(PANEL)
    cells, history = flow_blocks.shape[1:]
    width = interp_weights.shape[1]
    slots = donor_block.shape[0]
    owner = donor_owner[:, 0]

    row = jnp.arange(slots, dtype=jnp.int32)
    same = (owner[:, None] == owner[None, :]) & (row[None, :] < row[:, None])
    rank = jnp.sum(same.astype(jnp.int32), axis=1)
    slot = owner * CAP + rank
    slot_ids = jnp.arange(peers * CAP, dtype=jnp.int32)
    chosen = slot[:, None] == slot_ids[None, :]
    requests = jnp.sum(jnp.where(chosen, donor_block[:, None], 0), axis=0).reshape(peers, CAP)
    asked = lax.all_to_all(requests, PANEL, 0, 0, tiled=True)
    found = flow_blocks.at[asked.reshape(-1)].get(mode="promise_in_bounds")
    found = found.reshape(peers, CAP, cells, history)
    arrived = lax.all_to_all(found, PANEL, 0, 0, tiled=True)

    observers = lax.all_gather(lax.optimization_barrier((observer_points, asked))[0], "x", axis=1, tiled=True)
    basis, cosines, sines = geometry(panel_points.T, observers)
    table = fourier_table(NT, HARM)
    placing = chosen.astype(jnp.bfloat16)
    weights = interp_weights.reshape(width, slots, cells)
    placed = jnp.einsum("prc,rs->psc", weights, placing, preferred_element_type=jnp.float32)
    placed = placed.astype(jnp.bfloat16).reshape(width, peers * CAP * cells)

    values = jnp.dot(placed, arrived.reshape(-1, history), preferred_element_type=jnp.float32)
    partial = radiate(values, panel_normals.T, table, basis, cosines, sines)

    far, near, across = lax.axis_size("z"), lax.axis_size(("y", "c")), lax.axis_size("x")
    parts = partial.reshape(far, near, across, -1).transpose(1, 2, 0, 3).reshape(near * across, far, -1)
    parts = jnp.sum(lax.all_to_all(parts, SLAB, 0, 0, tiled=True), axis=0)
    parts = lax.all_to_all(parts.reshape(far, 1, -1), "z", 0, 0, tiled=True)
    return jnp.sum(parts, axis=0)


def solution(mesh):
    panel, obs = mesh.shape["panel"], mesh.shape["obs"]
    finer = Mesh(mesh.devices.reshape(panel // 8, 4, 2, obs), ("z", "y", "c", "x"))
    every = PANEL + ("x",)
    in_specs = (
        P(PANEL, None, None),
        P(every, None, None),
        P(every, None),
        P(every),
        P(None, every),
        P(None, every),
        P(None, "x"),
    )
    return jax.shard_map(body, mesh=finer, in_specs=in_specs, out_specs=P(PANEL, "x"), check_vma=False)
```

```python
import functools
import math

import jax
import jax.numpy as jnp
from jax import lax
from jax.experimental import pallas as pl
from jax.experimental.pallas import tpu as pltpu
from jax.sharding import Mesh
from jax.sharding import PartitionSpec as P

NV = 5
NT = 256
HARM = 64
KAPPA = 0.5
PANEL = ("z", "y", "c")
SLAB = ("y", "c", "x")
CAP = 2
GROUP = 8
PANEL_STEP = 32
TOGETHER = 4
OBS_TILE = 256


def harmonic_of(index):
    return (index % GROUP) * (HARM // GROUP) + index // GROUP + 1


def fourier_table(samples, orders):
    sample_ids = jnp.arange(samples, dtype=jnp.int32)
    harmonic = harmonic_of(jnp.arange(orders, dtype=jnp.int32))
    wrapped = sample_ids[:, None] * harmonic[None, :] % samples
    angles = wrapped.astype(jnp.float32) * (2.0 * math.pi / samples)
    factor = 2.0 / samples
    return jnp.concatenate([factor * jnp.cos(angles), -factor * jnp.sin(angles)], axis=1)


def geometry_kernel(points_ref, observers_ref, basis_ref, cos_ref, sin_ref):
    panels = points_ref.shape[0]
    offsets = [observers_ref[i : i + 1, :] - points_ref[:, i : i + 1] for i in range(3)]
    distance = jnp.sqrt(offsets[0] * offsets[0] + offsets[1] * offsets[1] + offsets[2] * offsets[2])
    inverse = 1.0 / distance
    weight = inverse * (1.0 / (4.0 * math.pi))
    near = weight * inverse
    rows = lambda j: pl.ds(j, panels, stride=GROUP)
    for i in range(3):
        direction = offsets[i] * inverse
        basis_ref[rows(i), :] = direction * near
        basis_ref[rows(3 + i), :] = direction * weight
    basis_ref[rows(6), :] = weight
    basis_ref[rows(7), :] = jnp.zeros_like(weight)
    phase = KAPPA * distance
    c, s = jnp.cos(phase), jnp.sin(phase)
    c8, s8 = c, s
    for _ in range(3):
        c8, s8 = c8 * c8 - s8 * s8, 2.0 * (s8 * c8)
    for j in range(GROUP):
        cos_ref[rows(j), :] = c
        sin_ref[rows(j), :] = s
        c, s = c * c8 - s * s8, s * c8 + c * s8


def geometry(points, observers):
    panels, total = points.shape[0], observers.shape[1]
    tile = 128
    shape = jax.ShapeDtypeStruct((panels * GROUP, total), jnp.float32)
    spec = pl.BlockSpec((panels * GROUP, tile), lambda x: (0, x))
    return pl.pallas_call(
        geometry_kernel,
        grid=(total // tile,),
        out_shape=(shape, shape, shape),
        in_specs=[
            pl.BlockSpec((panels, 3), lambda x: (0, 0)),
            pl.BlockSpec((3, tile), lambda x: (0, x)),
        ],
        out_specs=(spec, spec, spec),
        cost_estimate=pl.CostEstimate(
            flops=200 * panels * total, bytes_accessed=12 * panels * GROUP * total, transcendentals=3 * panels * total
        ),
        name="geometry",
    )(points, observers)


def split_two(value):
    high = value.astype(jnp.bfloat16).astype(jnp.float32)
    return high, value - high


def fill_factors(weights_ref, donors_ref, normals_ref, table_ref, factors_ref):
    slots, pairs, rows8, lanes128 = donors_ref.shape
    panels = normals_ref.shape[0]
    columns = []
    for t in range(pairs):
        block = donors_ref[:, t].reshape(slots * rows8, lanes128)
        both = jnp.dot(weights_ref[...], block, preferred_element_type=jnp.float32)
        columns += [both[:panels], both[panels:]]
    per = NT // lanes128
    field = lambda v: jnp.concatenate(columns[v * per : (v + 1) * per], axis=1)
    normal = [normals_ref[:, i : i + 1] for i in range(3)]
    flow = field(1) * normal[0] + field(2) * normal[1] + field(3) * normal[2]
    mass = (1.0 + field(0)) * flow
    loads = [field(4) * normal[i] + mass * field(1 + i) for i in range(3)]
    series = jnp.concatenate([mass] + loads, axis=0)
    spectra = jnp.dot(series, table_ref[...], precision=lax.Precision.HIGHEST, preferred_element_type=jnp.float32)
    lane = lax.broadcasted_iota(jnp.int32, (panels, 2 * HARM), 1)
    order = harmonic_of(jnp.where(lane < HARM, lane, lane - HARM)).astype(jnp.float32) * KAPPA
    wave = jnp.where(lane < HARM, -order, order)
    rows = lambda j: pl.ds(j, panels, stride=GROUP)
    for i in range(4):
        part = spectra[i * panels : (i + 1) * panels]
        turned = jnp.concatenate([part[:, HARM:], part[:, :HARM]], axis=1) * wave
        if i == 0:
            factors_ref[rows(6), :] = turned
        else:
            factors_ref[rows(i - 1), :] = part
            factors_ref[rows(2 + i), :] = turned
    factors_ref[rows(7), :] = jnp.zeros((panels, 2 * HARM), jnp.float32)


def left_factors(first, factors_ref):
    lefts = []
    for k in range(TOGETHER):
        high, low = split_two(factors_ref[pl.ds(pl.multiple_of((first + k) * GROUP, GROUP), GROUP), :])
        lefts.append(jnp.concatenate([high, high, low, jnp.zeros_like(low)], axis=0).astype(jnp.bfloat16))
    return lefts


def amplitudes(first, lefts, lanes, basis_ref, amps_ref):
    for k in range(TOGETHER):
        at = pl.multiple_of((first + k) * GROUP, GROUP)
        high, low = split_two(basis_ref[pl.ds(at, GROUP), lanes])
        right = jnp.concatenate([high, low, high, jnp.zeros_like(low)], axis=0).astype(jnp.bfloat16)
        amps_ref[k, :, lanes] = lax.dot_general(
            lefts[k], right, (((0,), (0,)), ((), ())), preferred_element_type=jnp.float32
        )


def add_up(first, lanes, amps_ref, cos_ref, sin_ref, sent_ref):
    width = sent_ref.shape[2]
    block, inner = lanes.start // width, slice(lanes.start % width, lanes.start % width + 128)
    across = cos_ref.shape[1] // width
    states = []
    for k in range(TOGETHER):
        at = pl.multiple_of((first + k) * GROUP, GROUP)
        c, s = cos_ref[pl.ds(at, GROUP), lanes], sin_ref[pl.ds(at, GROUP), lanes]
        c1 = jnp.broadcast_to(c[0:1, :], c.shape)
        s1 = jnp.broadcast_to(s[0:1, :], s.shape)
        states.append((c, s, c * c1 + s * s1, s * c1 - c * s1, 2.0 * c1))
    for r in range(HARM // GROUP):
        re = slice(r * GROUP, (r + 1) * GROUP)
        im = slice(HARM + r * GROUP, HARM + (r + 1) * GROUP)
        place = r * across + block
        total_re, total_im = sent_ref[place, 0:GROUP, inner], sent_ref[place, GROUP : 2 * GROUP, inner]
        for k in range(TOGETHER):
            c, s, before_c, before_s, twice = states[k]
            a_re, a_im = amps_ref[k, re, lanes], amps_ref[k, im, lanes]
            total_re = total_re + (a_re * c + a_im * s)
            total_im = total_im + (a_im * c - a_re * s)
            states[k] = (twice * c - before_c, twice * s - before_s, c, s, twice)
        sent_ref[place, 0:GROUP, inner] = total_re
        sent_ref[place, GROUP : 2 * GROUP, inner] = total_im


def radiate_kernel(
    weights_ref,
    donors_ref,
    normals_ref,
    table_ref,
    basis_ref,
    cos_ref,
    sin_ref,
    sent_ref,
    factors_ref,
    even_ref,
    odd_ref,
):
    step = pl.program_id(0)

    @pl.when(step == 0)
    def _():
        fill_factors(weights_ref, donors_ref, normals_ref, table_ref, factors_ref)
        sent_ref[...] = jnp.zeros_like(sent_ref)

    panel = step * PANEL_STEP
    last = PANEL_STEP - TOGETHER
    observers = basis_ref.shape[1]
    tiles = [slice(x, x + OBS_TILE) for x in range(0, observers, OBS_TILE)]
    parts = [slice(x, x + 128) for x in range(0, observers, 128)]

    lefts = left_factors(panel, factors_ref)
    for lanes in tiles:
        amplitudes(0, lefts, lanes, basis_ref, even_ref)

    def one_group(turn, carry):
        first = turn * TOGETHER
        following = jnp.minimum(first + TOGETHER, last)

        def compute(now_ref, next_ref):
            lefts = left_factors(panel + following, factors_ref)
            share = len(parts) // (len(tiles) + 1)
            done = 0
            for n, lanes in enumerate(tiles):
                for part in parts[done : done + share]:
                    add_up(first, part, now_ref, cos_ref, sin_ref, sent_ref)
                done += share
                amplitudes(following, lefts, lanes, basis_ref, next_ref)
            for part in parts[done:]:
                add_up(first, part, now_ref, cos_ref, sin_ref, sent_ref)

        pl.when(turn % 2 == 0)(lambda: compute(even_ref, odd_ref))
        pl.when(turn % 2 == 1)(lambda: compute(odd_ref, even_ref))
        return carry

    lax.fori_loop(0, PANEL_STEP // TOGETHER, one_group, 0)


def radiate(weights, donors, normals, table, basis, cosines, sines, sent):
    panels, observers = normals.shape[0], basis.shape[1]
    whole = lambda a: pl.BlockSpec(a.shape, lambda p: (0,) * len(a.shape))
    rows = pl.BlockSpec((PANEL_STEP * GROUP, observers), lambda p: (p, 0))
    return pl.pallas_call(
        radiate_kernel,
        grid=(panels // PANEL_STEP,),
        out_shape=sent,
        in_specs=[whole(weights), whole(donors), whole(normals), whole(table), rows, rows, rows],
        out_specs=whole(sent),
        scratch_shapes=[
            pltpu.VMEM((panels * GROUP, 2 * HARM), jnp.float32),
            pltpu.VMEM((TOGETHER, 2 * HARM, observers), jnp.float32),
            pltpu.VMEM((TOGETHER, 2 * HARM, observers), jnp.float32),
        ],
        cost_estimate=pl.CostEstimate(
            flops=30 * panels * HARM * observers, bytes_accessed=12 * panels * GROUP * observers, transcendentals=0
        ),
        name="radiate",
    )(weights, donors, normals, table, basis, cosines, sines)


def gather_kernel(asked_ref, blocks_ref, found_ref):
    peers = found_ref.shape[0]
    first = pl.program_id(0) * peers
    for i in range(peers):
        word = asked_ref[first + i]
        found_ref[i, 0] = blocks_ref[word & 0xFFFF]
        found_ref[i, 1] = blocks_ref[word >> 16]


def gather(asked, blocks):
    peers, together = asked.shape[0], 16
    rest = blocks.shape[1:]
    return pl.pallas_call(
        gather_kernel,
        grid_spec=pltpu.PrefetchScalarGridSpec(
            num_scalar_prefetch=1,
            grid=(peers // together,),
            in_specs=[pl.BlockSpec(blocks.shape, lambda p, asked: (0, 0, 0, 0))],
            out_specs=pl.BlockSpec((together, CAP) + rest, lambda p, asked: (p, 0, 0, 0, 0)),
        ),
        out_shape=jax.ShapeDtypeStruct((peers, CAP) + rest, blocks.dtype),
        name="gather",
    )(asked, blocks)


def body(flow_blocks, interp_weights, donor_owner, donor_block, panel_normals, panel_points, observer_points):
    peers = lax.axis_size(PANEL)
    cells, history = flow_blocks.shape[1:]
    width = interp_weights.shape[1]
    slots = donor_block.shape[0]
    owner = donor_owner[:, 0]

    row = jnp.arange(slots, dtype=jnp.int32)
    same = (owner[:, None] == owner[None, :]) & (row[None, :] < row[:, None])
    rank = jnp.sum(same.astype(jnp.int32), axis=1)
    slot = owner * CAP + rank
    slot_ids = jnp.arange(peers * CAP, dtype=jnp.int32)
    chosen = slot[:, None] == slot_ids[None, :]
    held = flow_blocks.shape[0]
    word = jnp.where(rank == 0, donor_block, donor_block << 16)
    named = owner[:, None] == jnp.arange(peers, dtype=jnp.int32)[None, :]
    requests = jnp.sum(jnp.where(named, word[:, None], 0), axis=0)
    asked = lax.all_to_all(requests, PANEL, 0, 0, tiled=True)
    tiles = history // 256
    blocks = flow_blocks.reshape(held, cells, tiles, 2, 128).transpose(0, 2, 3, 1, 4).reshape(held, tiles, 2 * cells, 128)
    arrived = lax.all_to_all(gather(asked, blocks), PANEL, 0, 0, tiled=True).reshape(peers * CAP, tiles, 2 * cells, 128)

    observers = lax.all_gather(lax.optimization_barrier((observer_points, asked))[0], "x", axis=1, tiled=True)
    basis, cosines, sines = geometry(panel_points.T, observers)
    table = fourier_table(NT, HARM)
    placing = chosen.astype(jnp.bfloat16)
    weights = interp_weights.reshape(width, slots, cells)
    placed = jnp.einsum("prc,rs->psc", weights, placing, preferred_element_type=jnp.float32).astype(jnp.bfloat16)
    halves = jnp.eye(2, dtype=jnp.bfloat16)[:, None, None, :, None] * placed[None, :, :, None, :]
    halves = halves.reshape(2 * width, peers * CAP * 2 * cells)

    far, near, across = lax.axis_size("z"), lax.axis_size(("y", "c")), lax.axis_size("x")
    sent = jax.ShapeDtypeStruct((near * across, far, observer_points.shape[1]), jnp.float32)
    parts = radiate(halves, arrived, panel_normals.T, table, basis, cosines, sines, sent)
    parts = jnp.sum(lax.all_to_all(parts, SLAB, 0, 0, tiled=True), axis=0)
    parts = lax.all_to_all(parts.reshape(far, 1, -1), "z", 0, 0, tiled=True)
    return jnp.sum(parts, axis=0)


def solution(mesh):
    panel, obs = mesh.shape["panel"], mesh.shape["obs"]
    finer = Mesh(mesh.devices.reshape(panel // 8, 4, 2, obs), ("z", "y", "c", "x"))
    every = PANEL + ("x",)
    in_specs = (
        P(PANEL, None, None),
        P(every, None, None),
        P(every, None),
        P(every),
        P(None, every),
        P(None, every),
        P(None, "x"),
    )
    return jax.shard_map(body, mesh=finer, in_specs=in_specs, out_specs=P(PANEL, "x"), check_vma=False)
```

```python
import functools
import math

import jax
import jax.numpy as jnp
from jax import lax
from jax.experimental import pallas as pl
from jax.experimental.pallas import tpu as pltpu
from jax.sharding import Mesh
from jax.sharding import PartitionSpec as P

NV = 5
NT = 256
HARM = 64
KAPPA = 0.5
PANEL = ("z", "y", "c")
SLAB = ("y", "c", "x")
CAP = 2
GROUP = 8
PANEL_STEP = 32
TOGETHER = 4
OBS_TILE = 256


def harmonic_of(index):
    return (index % GROUP) * (HARM // GROUP) + index // GROUP + 1


def fourier_table(samples, orders):
    sample_ids = jnp.arange(samples, dtype=jnp.int32)
    harmonic = harmonic_of(jnp.arange(orders, dtype=jnp.int32))
    wrapped = sample_ids[:, None] * harmonic[None, :] % samples
    angles = wrapped.astype(jnp.float32) * (2.0 * math.pi / samples)
    factor = 2.0 / samples
    return jnp.concatenate([factor * jnp.cos(angles), -factor * jnp.sin(angles)], axis=1)


def geometry_kernel(points_ref, observers_ref, made_ref):
    basis_ref, cos_ref, sin_ref = (made_ref.at[n] for n in range(3))
    panels = points_ref.shape[0]
    offsets = [observers_ref[i : i + 1, :] - points_ref[:, i : i + 1] for i in range(3)]
    distance = jnp.sqrt(offsets[0] * offsets[0] + offsets[1] * offsets[1] + offsets[2] * offsets[2])
    inverse = 1.0 / distance
    weight = inverse * (1.0 / (4.0 * math.pi))
    near = weight * inverse
    rows = lambda j: pl.ds(j, panels, stride=GROUP)
    for i in range(3):
        direction = offsets[i] * inverse
        basis_ref[rows(i), :] = direction * near
        basis_ref[rows(3 + i), :] = direction * weight
    basis_ref[rows(6), :] = weight
    basis_ref[rows(7), :] = jnp.zeros_like(weight)
    phase = KAPPA * distance
    c, s = jnp.cos(phase), jnp.sin(phase)
    c8, s8 = c, s
    for _ in range(3):
        c8, s8 = c8 * c8 - s8 * s8, 2.0 * (s8 * c8)
    for j in range(GROUP):
        cos_ref[rows(j), :] = c
        sin_ref[rows(j), :] = s
        c, s = c * c8 - s * s8, s * c8 + c * s8


def geometry(points, observers):
    panels, total = points.shape[0], observers.shape[1]
    tile = 128
    return pl.pallas_call(
        geometry_kernel,
        grid=(total // tile,),
        out_shape=jax.ShapeDtypeStruct((3, panels * GROUP, total), jnp.float32),
        in_specs=[
            pl.BlockSpec((panels, 3), lambda x: (0, 0)),
            pl.BlockSpec((3, tile), lambda x: (0, x)),
        ],
        out_specs=pl.BlockSpec((3, panels * GROUP, tile), lambda x: (0, 0, x)),
        cost_estimate=pl.CostEstimate(
            flops=200 * panels * total, bytes_accessed=12 * panels * GROUP * total, transcendentals=3 * panels * total
        ),
        name="geometry",
    )(points, observers)


def split_two(value):
    high = value.astype(jnp.bfloat16).astype(jnp.float32)
    return high, value - high


def fill_factors(weights_ref, donors_ref, normals_ref, table_ref, factors_ref):
    slots, pairs, rows8, lanes128 = donors_ref.shape
    panels = normals_ref.shape[0]
    columns = []
    for t in range(pairs):
        block = donors_ref[:, t].reshape(slots * rows8, lanes128)
        both = jnp.dot(weights_ref[...], block, preferred_element_type=jnp.float32)
        columns += [both[:panels], both[panels:]]
    per = NT // lanes128
    field = lambda v: jnp.concatenate(columns[v * per : (v + 1) * per], axis=1)
    normal = [normals_ref[:, i : i + 1] for i in range(3)]
    flow = field(1) * normal[0] + field(2) * normal[1] + field(3) * normal[2]
    mass = (1.0 + field(0)) * flow
    loads = [field(4) * normal[i] + mass * field(1 + i) for i in range(3)]
    series = jnp.concatenate([mass] + loads, axis=0)
    spectra = jnp.dot(series, table_ref[...], precision=lax.Precision.HIGHEST, preferred_element_type=jnp.float32)
    lane = lax.broadcasted_iota(jnp.int32, (panels, 2 * HARM), 1)
    order = harmonic_of(jnp.where(lane < HARM, lane, lane - HARM)).astype(jnp.float32) * KAPPA
    wave = jnp.where(lane < HARM, -order, order)
    rows = lambda j: pl.ds(j, panels, stride=GROUP)
    for i in range(4):
        part = spectra[i * panels : (i + 1) * panels]
        turned = jnp.concatenate([part[:, HARM:], part[:, :HARM]], axis=1) * wave
        if i == 0:
            factors_ref[rows(6), :] = turned
        else:
            factors_ref[rows(i - 1), :] = part
            factors_ref[rows(2 + i), :] = turned
    factors_ref[rows(7), :] = jnp.zeros((panels, 2 * HARM), jnp.float32)


def left_factors(first, factors_ref):
    lefts = []
    for k in range(TOGETHER):
        high, low = split_two(factors_ref[pl.ds(pl.multiple_of((first + k) * GROUP, GROUP), GROUP), :])
        lefts.append(jnp.concatenate([high, high, low, jnp.zeros_like(low)], axis=0).astype(jnp.bfloat16))
    return lefts


def amplitudes(first, lefts, lanes, basis_ref, amps_ref):
    for k in range(TOGETHER):
        at = pl.multiple_of((first + k) * GROUP, GROUP)
        high, low = split_two(basis_ref[pl.ds(at, GROUP), lanes])
        right = jnp.concatenate([high, low, high, jnp.zeros_like(low)], axis=0).astype(jnp.bfloat16)
        amps_ref[k, :, lanes] = lax.dot_general(
            lefts[k], right, (((0,), (0,)), ((), ())), preferred_element_type=jnp.float32
        )


def add_up(first, lanes, amps_ref, cos_ref, sin_ref, sent_ref):
    width = sent_ref.shape[2]
    block, inner = lanes.start // width, slice(lanes.start % width, lanes.start % width + 128)
    across = cos_ref.shape[1] // width
    states = []
    for k in range(TOGETHER):
        at = pl.multiple_of((first + k) * GROUP, GROUP)
        c, s = cos_ref[pl.ds(at, GROUP), lanes], sin_ref[pl.ds(at, GROUP), lanes]
        c1 = jnp.broadcast_to(c[0:1, :], c.shape)
        s1 = jnp.broadcast_to(s[0:1, :], s.shape)
        states.append((c, s, c * c1 + s * s1, s * c1 - c * s1, 2.0 * c1))
    for r in range(HARM // GROUP):
        re = slice(r * GROUP, (r + 1) * GROUP)
        im = slice(HARM + r * GROUP, HARM + (r + 1) * GROUP)
        place = r * across + block
        total_re, total_im = sent_ref[place, 0:GROUP, inner], sent_ref[place, GROUP : 2 * GROUP, inner]
        for k in range(TOGETHER):
            c, s, before_c, before_s, twice = states[k]
            a_re, a_im = amps_ref[k, re, lanes], amps_ref[k, im, lanes]
            total_re = total_re + (a_re * c + a_im * s)
            total_im = total_im + (a_im * c - a_re * s)
            states[k] = (twice * c - before_c, twice * s - before_s, c, s, twice)
        sent_ref[place, 0:GROUP, inner] = total_re
        sent_ref[place, GROUP : 2 * GROUP, inner] = total_im


def radiate_kernel(
    weights_ref,
    donors_ref,
    normals_ref,
    table_ref,
    made_hbm,
    sent_ref,
    made_ref,
    factors_ref,
    even_ref,
    odd_ref,
    arrived,
):
    size = PANEL_STEP * GROUP
    basis_ref, cos_ref, sin_ref = (made_ref.at[n] for n in range(3))

    def fetch(chunk):
        rows = pl.ds(pl.multiple_of(chunk * size, size), size)
        return pltpu.make_async_copy(made_hbm.at[:, rows, :], made_ref.at[:, rows, :], arrived.at[chunk])

    panels = normals_ref.shape[0]
    for chunk in range(panels // PANEL_STEP):
        fetch(chunk).start()
    fill_factors(weights_ref, donors_ref, normals_ref, table_ref, factors_ref)
    sent_ref[...] = jnp.zeros_like(sent_ref)
    fetch(0).wait()

    last = panels - TOGETHER
    observers = basis_ref.shape[1]
    tiles = [slice(x, x + OBS_TILE) for x in range(0, observers, OBS_TILE)]
    parts = [slice(x, x + 128) for x in range(0, observers, 128)]

    lefts = left_factors(0, factors_ref)
    for lanes in tiles:
        amplitudes(0, lefts, lanes, basis_ref, even_ref)

    def one_group(turn, carry):
        first = turn * TOGETHER
        following = jnp.minimum(first + TOGETHER, last)
        due = (first + TOGETHER) // PANEL_STEP

        @pl.when(((first + TOGETHER) % PANEL_STEP == 0) & (first < last))
        def _():
            fetch(due).wait()

        def compute(now_ref, next_ref):
            lefts = left_factors(following, factors_ref)
            share = len(parts) // (len(tiles) + 1)
            done = 0
            for lanes in tiles:
                for part in parts[done : done + share]:
                    add_up(first, part, now_ref, cos_ref, sin_ref, sent_ref)
                done += share
                amplitudes(following, lefts, lanes, basis_ref, next_ref)
            for part in parts[done:]:
                add_up(first, part, now_ref, cos_ref, sin_ref, sent_ref)

        pl.when(turn % 2 == 0)(lambda: compute(even_ref, odd_ref))
        pl.when(turn % 2 == 1)(lambda: compute(odd_ref, even_ref))
        return carry

    lax.fori_loop(0, panels // TOGETHER, one_group, 0)


def radiate(weights, donors, normals, table, made, sent):
    panels, observers = normals.shape[0], made.shape[2]
    near, far = pl.BlockSpec(memory_space=pltpu.VMEM), pl.BlockSpec(memory_space=pltpu.HBM)
    amps = pltpu.VMEM((TOGETHER, 2 * HARM, observers), jnp.float32)
    return pl.pallas_call(
        radiate_kernel,
        out_shape=sent,
        in_specs=[near, near, near, near, far],
        out_specs=near,
        scratch_shapes=[
            pltpu.VMEM(made.shape, jnp.float32),
            pltpu.VMEM((panels * GROUP, 2 * HARM), jnp.float32),
            amps,
            amps,
            pltpu.SemaphoreType.DMA((panels // PANEL_STEP,)),
        ],
        compiler_params=pltpu.CompilerParams(vmem_limit_bytes=46 * 2**20),
        cost_estimate=pl.CostEstimate(
            flops=30 * panels * HARM * observers, bytes_accessed=12 * panels * GROUP * observers, transcendentals=0
        ),
        name="radiate",
    )(weights, donors, normals, table, made)


def gather_kernel(asked_ref, blocks_ref, found_ref, sent):
    peers = found_ref.shape[0]

    def one_peer(peer, carry):
        word = asked_ref[peer, 0, 0]
        pltpu.make_async_copy(blocks_ref.at[word & 0xFFFF], found_ref.at[peer, 0], sent).start()
        pltpu.make_async_copy(blocks_ref.at[word >> 16], found_ref.at[peer, 1], sent).start()
        return carry

    lax.fori_loop(0, peers, one_peer, 0, unroll=8)
    pltpu.make_async_copy(found_ref, found_ref, sent).wait()


def gather(asked, blocks):
    return pl.pallas_call(
        gather_kernel,
        in_specs=[pl.BlockSpec(memory_space=pltpu.SMEM), pl.BlockSpec(memory_space=pltpu.VMEM)],
        out_specs=pl.BlockSpec(memory_space=pltpu.HBM),
        out_shape=jax.ShapeDtypeStruct((asked.shape[0], CAP) + blocks.shape[1:], blocks.dtype),
        scratch_shapes=[pltpu.SemaphoreType.DMA],
        name="gather",
    )(asked, blocks)


def body(flow_blocks, interp_weights, donor_owner, donor_block, panel_normals, panel_points, observer_points):
    peers = lax.axis_size(PANEL)
    cells, history = flow_blocks.shape[1:]
    width = interp_weights.shape[1]
    slots = donor_block.shape[0]
    owner = donor_owner[:, 0]

    held = flow_blocks.shape[0]
    named = owner[:, None] == jnp.arange(peers, dtype=jnp.int32)[None, :]
    lower = jnp.min(jnp.where(named, donor_block[:, None], held), axis=0)
    higher = jnp.max(jnp.where(named, donor_block[:, None], 0), axis=0)
    requests = jnp.where(lower == held, 0, lower) + (higher << 16)
    requests = lax.optimization_barrier(requests)
    asked = lax.all_to_all(requests.reshape(peers, 1, 1), PANEL, 0, 0, tiled=True)
    tiles = history // 256
    blocks = flow_blocks.reshape(held, cells, tiles, 2, 128).transpose(0, 2, 3, 1, 4).reshape(held, tiles, 2 * cells, 128)
    arrived = lax.all_to_all(gather(asked, blocks), PANEL, 0, 0, tiled=True).reshape(peers * CAP, tiles, 2 * cells, 128)

    observers = lax.all_gather(lax.optimization_barrier((observer_points, asked))[0], "x", axis=1, tiled=True)
    made = geometry(panel_points.T, observers)
    table = fourier_table(NT, HARM)
    row = jnp.arange(slots, dtype=jnp.int32)
    key = donor_block * slots + row
    rank = jnp.sum(((owner[:, None] == owner[None, :]) & (key[None, :] < key[:, None])).astype(jnp.int32), axis=1)
    chosen = (owner * CAP + rank)[:, None] == jnp.arange(peers * CAP, dtype=jnp.int32)[None, :]
    placing = chosen.astype(jnp.bfloat16)
    weights = interp_weights.reshape(width, slots, cells)
    placed = jnp.einsum("prc,rs->psc", weights, placing, preferred_element_type=jnp.float32).astype(jnp.bfloat16)
    halves = jnp.eye(2, dtype=jnp.bfloat16)[:, None, None, :, None] * placed[None, :, :, None, :]
    halves = halves.reshape(2 * width, peers * CAP * 2 * cells)

    far, near, across = lax.axis_size("z"), lax.axis_size(("y", "c")), lax.axis_size("x")
    sent = jax.ShapeDtypeStruct((near * across, far, observer_points.shape[1]), jnp.float32)
    parts = radiate(halves, arrived, panel_normals.T, table, made, sent)
    parts = jnp.sum(lax.all_to_all(parts, SLAB, 0, 0, tiled=True), axis=0)
    parts = lax.all_to_all(parts.reshape(far, 1, -1), "z", 0, 0, tiled=True)
    return jnp.sum(parts, axis=0)


def solution(mesh):
    panel, obs = mesh.shape["panel"], mesh.shape["obs"]
    finer = Mesh(mesh.devices.reshape(panel // 8, 4, 2, obs), ("z", "y", "c", "x"))
    every = PANEL + ("x",)
    in_specs = (
        P(PANEL, None, None),
        P(every, None, None),
        P(every, None),
        P(every),
        P(None, every),
        P(None, every),
        P(None, "x"),
    )
    return jax.shard_map(body, mesh=finer, in_specs=in_specs, out_specs=P(PANEL, "x"), check_vma=False)
```

```python
import functools
import math

import jax
import jax.numpy as jnp
from jax import lax
from jax.experimental import pallas as pl
from jax.experimental.pallas import tpu as pltpu
from jax.sharding import Mesh
from jax.sharding import PartitionSpec as P

NV = 5
NT = 256
HARM = 64
KAPPA = 0.5
PANEL = ("z", "y", "c")
SLAB = ("y", "c", "x")
CAP = 2
GROUP = 8
PANEL_STEP = 32
TOGETHER = 4
OBS_TILE = 256


def harmonic_of(index):
    return (index % GROUP) * (HARM // GROUP) + index // GROUP + 1


def fourier_table(samples, orders):
    sample_ids = jnp.arange(samples, dtype=jnp.int32)
    harmonic = harmonic_of(jnp.arange(orders, dtype=jnp.int32))
    wrapped = sample_ids[:, None] * harmonic[None, :] % samples
    angles = wrapped.astype(jnp.float32) * (2.0 * math.pi / samples)
    factor = 2.0 / samples
    return jnp.concatenate([factor * jnp.cos(angles), -factor * jnp.sin(angles)], axis=1)


def geometry_kernel(points_ref, observers_ref, made_ref):
    basis_ref, cos_ref, sin_ref = (made_ref.at[n] for n in range(3))
    panels = points_ref.shape[0]
    offsets = [observers_ref[i : i + 1, :] - points_ref[:, i : i + 1] for i in range(3)]
    distance = jnp.sqrt(offsets[0] * offsets[0] + offsets[1] * offsets[1] + offsets[2] * offsets[2])
    inverse = 1.0 / distance
    weight = inverse * (1.0 / (4.0 * math.pi))
    near = weight * inverse
    rows = lambda j: pl.ds(j, panels, stride=GROUP)
    for i in range(3):
        direction = offsets[i] * inverse
        basis_ref[rows(i), :] = direction * near
        basis_ref[rows(3 + i), :] = direction * weight
    basis_ref[rows(6), :] = weight
    basis_ref[rows(7), :] = jnp.zeros_like(weight)
    phase = KAPPA * distance
    c, s = jnp.cos(phase), jnp.sin(phase)
    c8, s8 = c, s
    for _ in range(3):
        c8, s8 = c8 * c8 - s8 * s8, 2.0 * (s8 * c8)
    for j in range(GROUP):
        cos_ref[rows(j), :] = c
        sin_ref[rows(j), :] = s
        c, s = c * c8 - s * s8, s * c8 + c * s8


def geometry(points, observers):
    panels, total = points.shape[0], observers.shape[1]
    tile = 128
    return pl.pallas_call(
        geometry_kernel,
        grid=(total // tile,),
        out_shape=jax.ShapeDtypeStruct((3, panels * GROUP, total), jnp.float32),
        in_specs=[
            pl.BlockSpec((panels, 3), lambda x: (0, 0)),
            pl.BlockSpec((3, tile), lambda x: (0, x)),
        ],
        out_specs=pl.BlockSpec((3, panels * GROUP, tile), lambda x: (0, 0, x)),
        cost_estimate=pl.CostEstimate(
            flops=200 * panels * total, bytes_accessed=12 * panels * GROUP * total, transcendentals=3 * panels * total
        ),
        name="geometry",
    )(points, observers)


def split_two(value):
    high = value.astype(jnp.bfloat16).astype(jnp.float32)
    return high, value - high


def fill_factors(weights_ref, donors_ref, normals_ref, table_ref, factors_ref):
    slots, pairs, rows8, lanes128 = donors_ref.shape
    panels = normals_ref.shape[0]
    columns = []
    for t in range(pairs):
        block = donors_ref[:, t].reshape(slots * rows8, lanes128)
        both = jnp.dot(weights_ref[...], block, preferred_element_type=jnp.float32)
        columns += [both[:panels], both[panels:]]
    per = NT // lanes128
    field = lambda v: jnp.concatenate(columns[v * per : (v + 1) * per], axis=1)
    normal = [normals_ref[:, i : i + 1] for i in range(3)]
    flow = field(1) * normal[0] + field(2) * normal[1] + field(3) * normal[2]
    mass = (1.0 + field(0)) * flow
    loads = [field(4) * normal[i] + mass * field(1 + i) for i in range(3)]
    series = jnp.concatenate([mass] + loads, axis=0)
    spectra = jnp.dot(series, table_ref[...], precision=lax.Precision.HIGHEST, preferred_element_type=jnp.float32)
    lane = lax.broadcasted_iota(jnp.int32, (panels, 2 * HARM), 1)
    order = harmonic_of(jnp.where(lane < HARM, lane, lane - HARM)).astype(jnp.float32) * KAPPA
    wave = jnp.where(lane < HARM, -order, order)
    rows = lambda j: pl.ds(j, panels, stride=GROUP)
    for i in range(4):
        part = spectra[i * panels : (i + 1) * panels]
        turned = jnp.concatenate([part[:, HARM:], part[:, :HARM]], axis=1) * wave
        if i == 0:
            factors_ref[rows(6), :] = turned
        else:
            factors_ref[rows(i - 1), :] = part
            factors_ref[rows(2 + i), :] = turned
    factors_ref[rows(7), :] = jnp.zeros((panels, 2 * HARM), jnp.float32)


def left_factors(first, factors_ref):
    lefts = []
    for k in range(TOGETHER):
        high, low = split_two(factors_ref[pl.ds(pl.multiple_of((first + k) * GROUP, GROUP), GROUP), :])
        lefts.append(jnp.concatenate([high, high, low, jnp.zeros_like(low)], axis=0).astype(jnp.bfloat16))
    return lefts


def amplitudes(first, lefts, lanes, basis_ref, amps_ref):
    for k in range(TOGETHER):
        at = pl.multiple_of((first + k) * GROUP, GROUP)
        high, low = split_two(basis_ref[pl.ds(at, GROUP), lanes])
        right = jnp.concatenate([high, low, high, jnp.zeros_like(low)], axis=0).astype(jnp.bfloat16)
        amps_ref[k, :, lanes] = lax.dot_general(
            lefts[k], right, (((0,), (0,)), ((), ())), preferred_element_type=jnp.float32
        )


def add_up(first, lanes, amps_ref, cos_ref, sin_ref, sent_ref):
    width = sent_ref.shape[2]
    block, inner = lanes.start // width, slice(lanes.start % width, lanes.start % width + 128)
    across = cos_ref.shape[1] // width
    states = []
    for k in range(TOGETHER):
        at = pl.multiple_of((first + k) * GROUP, GROUP)
        c, s = cos_ref[pl.ds(at, GROUP), lanes], sin_ref[pl.ds(at, GROUP), lanes]
        c1 = jnp.broadcast_to(c[0:1, :], c.shape)
        s1 = jnp.broadcast_to(s[0:1, :], s.shape)
        states.append((c, s, c * c1 + s * s1, s * c1 - c * s1, 2.0 * c1))
    for r in range(HARM // GROUP):
        re = slice(r * GROUP, (r + 1) * GROUP)
        im = slice(HARM + r * GROUP, HARM + (r + 1) * GROUP)
        place = r * across + block
        total_re, total_im = sent_ref[place, 0:GROUP, inner], sent_ref[place, GROUP : 2 * GROUP, inner]
        for k in range(TOGETHER):
            c, s, before_c, before_s, twice = states[k]
            a_re, a_im = amps_ref[k, re, lanes], amps_ref[k, im, lanes]
            total_re = total_re + (a_re * c + a_im * s)
            total_im = total_im + (a_im * c - a_re * s)
            states[k] = (twice * c - before_c, twice * s - before_s, c, s, twice)
        sent_ref[place, 0:GROUP, inner] = total_re
        sent_ref[place, GROUP : 2 * GROUP, inner] = total_im


def radiate_kernel(
    weights_ref,
    donors_ref,
    normals_ref,
    table_ref,
    made_hbm,
    sent_ref,
    made_ref,
    factors_ref,
    even_ref,
    odd_ref,
    arrived,
):
    size = PANEL_STEP * GROUP
    basis_ref, cos_ref, sin_ref = (made_ref.at[n] for n in range(3))

    def fetch(chunk):
        rows = pl.ds(pl.multiple_of(chunk * size, size), size)
        return pltpu.make_async_copy(made_hbm.at[:, rows, :], made_ref.at[:, rows, :], arrived.at[chunk])

    panels = normals_ref.shape[0]
    for chunk in range(panels // PANEL_STEP):
        fetch(chunk).start()
    fill_factors(weights_ref, donors_ref, normals_ref, table_ref, factors_ref)
    sent_ref[...] = jnp.zeros_like(sent_ref)
    fetch(0).wait()

    last = panels - TOGETHER
    observers = basis_ref.shape[1]
    tiles = [slice(x, x + OBS_TILE) for x in range(0, observers, OBS_TILE)]
    parts = [slice(x, x + 128) for x in range(0, observers, 128)]

    lefts = left_factors(0, factors_ref)
    for lanes in tiles:
        amplitudes(0, lefts, lanes, basis_ref, even_ref)

    def one_group(turn, carry):
        first = turn * TOGETHER
        following = jnp.minimum(first + TOGETHER, last)
        due = (first + TOGETHER) // PANEL_STEP

        @pl.when(((first + TOGETHER) % PANEL_STEP == 0) & (first < last))
        def _():
            fetch(due).wait()

        def compute(now_ref, next_ref):
            lefts = left_factors(following, factors_ref)
            share = len(parts) // (len(tiles) + 1)
            done = 0
            for lanes in tiles:
                for part in parts[done : done + share]:
                    add_up(first, part, now_ref, cos_ref, sin_ref, sent_ref)
                done += share
                amplitudes(following, lefts, lanes, basis_ref, next_ref)
            for part in parts[done:]:
                add_up(first, part, now_ref, cos_ref, sin_ref, sent_ref)

        pl.when(turn % 2 == 0)(lambda: compute(even_ref, odd_ref))
        pl.when(turn % 2 == 1)(lambda: compute(odd_ref, even_ref))
        return carry

    lax.fori_loop(0, panels // TOGETHER, one_group, 0)


def radiate(weights, donors, normals, table, made, sent):
    panels, observers = normals.shape[0], made.shape[2]
    near, far = pl.BlockSpec(memory_space=pltpu.VMEM), pl.BlockSpec(memory_space=pltpu.HBM)
    amps = pltpu.VMEM((TOGETHER, 2 * HARM, observers), jnp.float32)
    return pl.pallas_call(
        radiate_kernel,
        out_shape=sent,
        in_specs=[near, near, near, near, far],
        out_specs=near,
        scratch_shapes=[
            pltpu.VMEM(made.shape, jnp.float32),
            pltpu.VMEM((panels * GROUP, 2 * HARM), jnp.float32),
            amps,
            amps,
            pltpu.SemaphoreType.DMA((panels // PANEL_STEP,)),
        ],
        compiler_params=pltpu.CompilerParams(
            vmem_limit_bytes=46 * 2**20
        ),
        cost_estimate=pl.CostEstimate(
            flops=30 * panels * HARM * observers, bytes_accessed=12 * panels * GROUP * observers, transcendentals=0
        ),
        name="radiate",
    )(weights, donors, normals, table, made)


def gather_kernel(asked_ref, blocks_ref, found_ref, sent):
    peers = found_ref.shape[0]

    def one_peer(peer, carry):
        word = asked_ref[peer, 0, 0]
        pltpu.make_async_copy(blocks_ref.at[word & 0xFFFF], found_ref.at[peer, 0], sent).start()
        pltpu.make_async_copy(blocks_ref.at[word >> 16], found_ref.at[peer, 1], sent).start()
        return carry

    lax.fori_loop(0, peers, one_peer, 0, unroll=8)
    pltpu.make_async_copy(found_ref, found_ref, sent).wait()


def gather(asked, blocks):
    return pl.pallas_call(
        gather_kernel,
        in_specs=[pl.BlockSpec(memory_space=pltpu.SMEM), pl.BlockSpec(memory_space=pltpu.VMEM)],
        out_specs=pl.BlockSpec(memory_space=pltpu.HBM),
        out_shape=jax.ShapeDtypeStruct((asked.shape[0], CAP) + blocks.shape[1:], blocks.dtype),
        scratch_shapes=[pltpu.SemaphoreType.DMA],
        name="gather",
    )(asked, blocks)


def body(flow_blocks, interp_weights, donor_owner, donor_block, panel_normals, panel_points, observer_points):
    peers = lax.axis_size(PANEL)
    cells, history = flow_blocks.shape[1:]
    width = interp_weights.shape[1]
    slots = donor_block.shape[0]
    owner = donor_owner[:, 0]

    held = flow_blocks.shape[0]
    named = owner[:, None] == jnp.arange(peers, dtype=jnp.int32)[None, :]
    lower = jnp.min(jnp.where(named, donor_block[:, None], held), axis=0)
    higher = jnp.max(jnp.where(named, donor_block[:, None], 0), axis=0)
    requests = jnp.where(lower == held, 0, lower) + (higher << 16)
    requests = lax.optimization_barrier(requests)
    asked = lax.all_to_all(requests.reshape(peers, 1, 1), PANEL, 0, 0, tiled=True)
    tiles = history // 256
    blocks = flow_blocks.reshape(held, cells, tiles, 2, 128).transpose(0, 2, 3, 1, 4).reshape(held, tiles, 2 * cells, 128)
    arrived = lax.all_to_all(gather(asked, blocks), PANEL, 0, 0, tiled=True).reshape(peers * CAP, tiles, 2 * cells, 128)

    observer_points, owner, donor_block, _ = lax.optimization_barrier((observer_points, owner, donor_block, asked))
    observers = lax.all_gather(observer_points, "x", axis=1, tiled=True)
    made = geometry(panel_points.T, observers)
    table = fourier_table(NT, HARM)
    row = jnp.arange(slots, dtype=jnp.int32)
    key = donor_block * slots + row
    rank = jnp.sum(((owner[:, None] == owner[None, :]) & (key[None, :] < key[:, None])).astype(jnp.int32), axis=1)
    chosen = (owner * CAP + rank)[:, None] == jnp.arange(peers * CAP, dtype=jnp.int32)[None, :]
    placing = chosen.astype(jnp.bfloat16)
    weights = interp_weights.reshape(width, slots, cells)
    placed = jnp.einsum("prc,rs->psc", weights, placing, preferred_element_type=jnp.float32).astype(jnp.bfloat16)
    halves = jnp.eye(2, dtype=jnp.bfloat16)[:, None, None, :, None] * placed[None, :, :, None, :]
    halves = halves.reshape(2 * width, peers * CAP * 2 * cells)

    far, near, across = lax.axis_size("z"), lax.axis_size(("y", "c")), lax.axis_size("x")
    sent = jax.ShapeDtypeStruct((near * across, far, observer_points.shape[1]), jnp.float32)
    parts = radiate(halves, arrived, panel_normals.T, table, made, sent)
    parts = jnp.sum(lax.all_to_all(parts, SLAB, 0, 0, tiled=True), axis=0)
    parts = lax.all_to_all(parts.reshape(far, 1, -1), "z", 0, 0, tiled=True)
    return jnp.sum(parts, axis=0)


def solution(mesh):
    panel, obs = mesh.shape["panel"], mesh.shape["obs"]
    finer = Mesh(mesh.devices.reshape(panel // 8, 4, 2, obs), ("z", "y", "c", "x"))
    every = PANEL + ("x",)
    in_specs = (
        P(PANEL, None, None),
        P(every, None, None),
        P(every, None),
        P(every),
        P(None, every),
        P(None, every),
        P(None, "x"),
    )
    return jax.shard_map(body, mesh=finer, in_specs=in_specs, out_specs=P(PANEL, "x"), check_vma=False)
```

```python
import functools
import math

import jax
import jax.numpy as jnp
from jax import lax
from jax.experimental import pallas as pl
from jax.experimental.pallas import tpu as pltpu
from jax.sharding import Mesh
from jax.sharding import PartitionSpec as P

NV = 5
NT = 256
HARM = 64
KAPPA = 0.5
PANEL = ("z", "y", "c")
SLAB = ("y", "c", "x")
CAP = 2
GROUP = 8
PANEL_STEP = 16
TOGETHER = 4
OBS_TILE = 256


def harmonic_of(index):
    return (index % GROUP) * (HARM // GROUP) + index // GROUP + 1


def fourier_table(samples, orders):
    sample_ids = jnp.arange(samples, dtype=jnp.int32)
    harmonic = harmonic_of(jnp.arange(orders, dtype=jnp.int32))
    wrapped = sample_ids[:, None] * harmonic[None, :] % samples
    angles = wrapped.astype(jnp.float32) * (2.0 * math.pi / samples)
    factor = 2.0 / samples
    return jnp.concatenate([factor * jnp.cos(angles), -factor * jnp.sin(angles)], axis=1)


def geometry_kernel(points_ref, observers_ref, made_ref):
    basis_ref, cos_ref, sin_ref = (made_ref.at[n] for n in range(3))
    panels = points_ref.shape[0]
    offsets = [observers_ref[i : i + 1, :] - points_ref[:, i : i + 1] for i in range(3)]
    distance = jnp.sqrt(offsets[0] * offsets[0] + offsets[1] * offsets[1] + offsets[2] * offsets[2])
    inverse = 1.0 / distance
    weight = inverse * (1.0 / (4.0 * math.pi))
    near = weight * inverse
    rows = lambda j: pl.ds(j, panels, stride=GROUP)
    for i in range(3):
        direction = offsets[i] * inverse
        basis_ref[rows(i), :] = direction * near
        basis_ref[rows(3 + i), :] = direction * weight
    basis_ref[rows(6), :] = weight
    basis_ref[rows(7), :] = jnp.zeros_like(weight)
    phase = KAPPA * distance
    c, s = jnp.cos(phase), jnp.sin(phase)
    c8, s8 = c, s
    for _ in range(3):
        c8, s8 = c8 * c8 - s8 * s8, 2.0 * (s8 * c8)
    for j in range(GROUP):
        cos_ref[rows(j), :] = c
        sin_ref[rows(j), :] = s
        c, s = c * c8 - s * s8, s * c8 + c * s8


def geometry(points, observers):
    panels, total = points.shape[0], observers.shape[1]
    tile = 128
    return pl.pallas_call(
        geometry_kernel,
        grid=(total // tile,),
        out_shape=jax.ShapeDtypeStruct((3, panels * GROUP, total), jnp.float32),
        in_specs=[
            pl.BlockSpec((panels, 3), lambda x: (0, 0)),
            pl.BlockSpec((3, tile), lambda x: (0, x)),
        ],
        out_specs=pl.BlockSpec((3, panels * GROUP, tile), lambda x: (0, 0, x)),
        cost_estimate=pl.CostEstimate(
            flops=200 * panels * total, bytes_accessed=12 * panels * GROUP * total, transcendentals=3 * panels * total
        ),
        name="geometry",
    )(points, observers)


def split_two(value):
    high = value.astype(jnp.bfloat16).astype(jnp.float32)
    return high, value - high


def fill_factors(weights_ref, donors_ref, normals_ref, table_ref, factors_ref):
    slots, pairs, rows8, lanes128 = donors_ref.shape
    panels = normals_ref.shape[0]
    columns = []
    for t in range(pairs):
        block = donors_ref[:, t].reshape(slots * rows8, lanes128)
        both = jnp.dot(weights_ref[...], block, preferred_element_type=jnp.float32)
        columns += [both[:panels], both[panels:]]
    per = NT // lanes128
    field = lambda v: jnp.concatenate(columns[v * per : (v + 1) * per], axis=1)
    normal = [normals_ref[:, i : i + 1] for i in range(3)]
    flow = field(1) * normal[0] + field(2) * normal[1] + field(3) * normal[2]
    mass = (1.0 + field(0)) * flow
    loads = [field(4) * normal[i] + mass * field(1 + i) for i in range(3)]
    series = jnp.concatenate([mass] + loads, axis=0)
    spectra = jnp.dot(series, table_ref[...], precision=lax.Precision.HIGHEST, preferred_element_type=jnp.float32)
    lane = lax.broadcasted_iota(jnp.int32, (panels, 2 * HARM), 1)
    order = harmonic_of(jnp.where(lane < HARM, lane, lane - HARM)).astype(jnp.float32) * KAPPA
    wave = jnp.where(lane < HARM, -order, order)
    rows = lambda j: pl.ds(j, panels, stride=GROUP)
    for i in range(4):
        part = spectra[i * panels : (i + 1) * panels]
        turned = jnp.concatenate([part[:, HARM:], part[:, :HARM]], axis=1) * wave
        if i == 0:
            factors_ref[rows(6), :] = turned
        else:
            factors_ref[rows(i - 1), :] = part
            factors_ref[rows(2 + i), :] = turned
    factors_ref[rows(7), :] = jnp.zeros((panels, 2 * HARM), jnp.float32)


def left_factors(first, factors_ref):
    lefts = []
    for k in range(TOGETHER):
        high, low = split_two(factors_ref[pl.ds(pl.multiple_of((first + k) * GROUP, GROUP), GROUP), :])
        lefts.append(jnp.concatenate([high, high, low, jnp.zeros_like(low)], axis=0).astype(jnp.bfloat16))
    return lefts


def amplitudes(first, lefts, lanes, basis_ref, amps_ref):
    for k in range(TOGETHER):
        at = pl.multiple_of((first + k) * GROUP, GROUP)
        high, low = split_two(basis_ref[pl.ds(at, GROUP), lanes])
        right = jnp.concatenate([high, low, high, jnp.zeros_like(low)], axis=0).astype(jnp.bfloat16)
        amps_ref[k, :, lanes] = lax.dot_general(
            lefts[k], right, (((0,), (0,)), ((), ())), preferred_element_type=jnp.float32
        )


def add_up(first, lanes, amps_ref, cos_ref, sin_ref, sent_ref):
    width = sent_ref.shape[2]
    block, inner = lanes.start // width, slice(lanes.start % width, lanes.start % width + 128)
    across = cos_ref.shape[1] // width
    states = []
    for k in range(TOGETHER):
        at = pl.multiple_of((first + k) * GROUP, GROUP)
        c, s = cos_ref[pl.ds(at, GROUP), lanes], sin_ref[pl.ds(at, GROUP), lanes]
        c1 = jnp.broadcast_to(c[0:1, :], c.shape)
        s1 = jnp.broadcast_to(s[0:1, :], s.shape)
        states.append((c, s, c * c1 + s * s1, s * c1 - c * s1, 2.0 * c1))
    for r in range(HARM // GROUP):
        re = slice(r * GROUP, (r + 1) * GROUP)
        im = slice(HARM + r * GROUP, HARM + (r + 1) * GROUP)
        place = r * across + block
        total_re, total_im = sent_ref[place, 0:GROUP, inner], sent_ref[place, GROUP : 2 * GROUP, inner]
        for k in range(TOGETHER):
            c, s, before_c, before_s, twice = states[k]
            a_re, a_im = amps_ref[k, re, lanes], amps_ref[k, im, lanes]
            total_re = total_re + (a_re * c + a_im * s)
            total_im = total_im + (a_im * c - a_re * s)
            states[k] = (twice * c - before_c, twice * s - before_s, c, s, twice)
        sent_ref[place, 0:GROUP, inner] = total_re
        sent_ref[place, GROUP : 2 * GROUP, inner] = total_im


def radiate_kernel(
    weights_ref,
    donors_ref,
    normals_ref,
    table_ref,
    made_hbm,
    sent_ref,
    made_ref,
    factors_ref,
    even_ref,
    odd_ref,
    arrived,
):
    size = PANEL_STEP * GROUP
    basis_ref, cos_ref, sin_ref = (made_ref.at[n] for n in range(3))

    def fetch(chunk):
        rows = pl.ds(pl.multiple_of(chunk * size, size), size)
        return pltpu.make_async_copy(made_hbm.at[:, rows, :], made_ref.at[:, rows, :], arrived.at[chunk])

    panels = normals_ref.shape[0]
    for chunk in range(panels // PANEL_STEP):
        fetch(chunk).start()
    fill_factors(weights_ref, donors_ref, normals_ref, table_ref, factors_ref)
    sent_ref[...] = jnp.zeros_like(sent_ref)
    fetch(0).wait()

    last = panels - TOGETHER
    observers = basis_ref.shape[1]
    tiles = [slice(x, x + OBS_TILE) for x in range(0, observers, OBS_TILE)]
    parts = [slice(x, x + 128) for x in range(0, observers, 128)]

    lefts = left_factors(0, factors_ref)
    for lanes in tiles:
        amplitudes(0, lefts, lanes, basis_ref, even_ref)

    def one_group(turn, carry):
        first = turn * TOGETHER
        following = jnp.minimum(first + TOGETHER, last)
        due = (first + TOGETHER) // PANEL_STEP

        @pl.when(((first + TOGETHER) % PANEL_STEP == 0) & (first < last))
        def _():
            fetch(due).wait()

        def compute(now_ref, next_ref):
            lefts = left_factors(following, factors_ref)
            share = len(parts) // (len(tiles) + 1)
            done = 0
            for lanes in tiles:
                for part in parts[done : done + share]:
                    add_up(first, part, now_ref, cos_ref, sin_ref, sent_ref)
                done += share
                amplitudes(following, lefts, lanes, basis_ref, next_ref)
            for part in parts[done:]:
                add_up(first, part, now_ref, cos_ref, sin_ref, sent_ref)

        pl.when(turn % 2 == 0)(lambda: compute(even_ref, odd_ref))
        pl.when(turn % 2 == 1)(lambda: compute(odd_ref, even_ref))
        return carry

    lax.fori_loop(0, panels // TOGETHER, one_group, 0)


def radiate(weights, donors, normals, table, made, sent):
    panels, observers = normals.shape[0], made.shape[2]
    near, far = pl.BlockSpec(memory_space=pltpu.VMEM), pl.BlockSpec(memory_space=pltpu.HBM)
    amps = pltpu.VMEM((TOGETHER, 2 * HARM, observers), jnp.float32)
    return pl.pallas_call(
        radiate_kernel,
        out_shape=sent,
        in_specs=[near, near, near, near, far],
        out_specs=near,
        scratch_shapes=[
            pltpu.VMEM(made.shape, jnp.float32),
            pltpu.VMEM((panels * GROUP, 2 * HARM), jnp.float32),
            amps,
            amps,
            pltpu.SemaphoreType.DMA((panels // PANEL_STEP,)),
        ],
        compiler_params=pltpu.CompilerParams(
            vmem_limit_bytes=46 * 2**20
        ),
        cost_estimate=pl.CostEstimate(
            flops=30 * panels * HARM * observers, bytes_accessed=12 * panels * GROUP * observers, transcendentals=0
        ),
        name="radiate",
    )(weights, donors, normals, table, made)


def gather_kernel(asked_ref, blocks_ref, found_ref, sent):
    peers, last = found_ref.shape[0], blocks_ref.shape[0] - 1

    def one_peer(peer, carry):
        word = asked_ref[peer, 0, 0]
        pltpu.make_async_copy(blocks_ref.at[last - (word & 0xFFFF)], found_ref.at[peer, 0], sent).start()
        pltpu.make_async_copy(blocks_ref.at[last - (word >> 16)], found_ref.at[peer, 1], sent).start()
        return carry

    lax.fori_loop(0, peers, one_peer, 0, unroll=8)
    pltpu.make_async_copy(found_ref, found_ref, sent).wait()


def gather(asked, blocks):
    return pl.pallas_call(
        gather_kernel,
        in_specs=[pl.BlockSpec(memory_space=pltpu.SMEM), pl.BlockSpec(memory_space=pltpu.VMEM)],
        out_specs=pl.BlockSpec(memory_space=pltpu.HBM),
        out_shape=jax.ShapeDtypeStruct((asked.shape[0], CAP) + blocks.shape[1:], blocks.dtype),
        scratch_shapes=[pltpu.SemaphoreType.DMA],
        compiler_params=pltpu.CompilerParams(vmem_limit_bytes=16 * 2**20),
        name="gather",
    )(asked, blocks)


def body(flow_blocks, interp_weights, donor_owner, donor_block, panel_normals, panel_points, observer_points):
    peers = lax.axis_size(PANEL)
    cells, history = flow_blocks.shape[1:]
    width = interp_weights.shape[1]
    slots = donor_block.shape[0]
    owner = donor_owner[:, 0]

    held = flow_blocks.shape[0]
    named = owner[:, None] == jnp.arange(peers, dtype=jnp.int32)[None, :]
    lower = jnp.min(jnp.where(named, donor_block[:, None], held), axis=0)
    higher = jnp.max(jnp.where(named, donor_block[:, None], 0), axis=0)
    requests = jnp.where(lower == held, 0, lower) + (higher << 16)
    requests = lax.optimization_barrier(requests)
    asked = lax.all_to_all(requests.reshape(peers, 1, 1), PANEL, 0, 0, tiled=True)
    tiles = history // 256
    blocks = flow_blocks.reshape(held, cells, tiles, 2, 128).transpose(0, 2, 3, 1, 4).reshape(held, tiles, 2 * cells, 128)
    arrived = lax.all_to_all(gather(asked, jnp.flip(blocks, 0)), PANEL, 0, 0, tiled=True).reshape(peers * CAP, tiles, 2 * cells, 128)

    observer_points, owner, donor_block, _ = lax.optimization_barrier((observer_points, owner, donor_block, asked))
    observers = lax.all_gather(observer_points, "x", axis=1, tiled=True)
    made = geometry(panel_points.T, observers)
    table = fourier_table(NT, HARM)
    row = jnp.arange(slots, dtype=jnp.int32)
    key = donor_block * slots + row
    rank = jnp.sum(((owner[:, None] == owner[None, :]) & (key[None, :] < key[:, None])).astype(jnp.int32), axis=1)
    chosen = (owner * CAP + rank)[:, None] == jnp.arange(peers * CAP, dtype=jnp.int32)[None, :]
    placing = chosen.astype(jnp.bfloat16)
    weights = interp_weights.reshape(width, slots, cells)
    placed = jnp.einsum("prc,rs->psc", weights, placing, preferred_element_type=jnp.float32).astype(jnp.bfloat16)
    halves = jnp.eye(2, dtype=jnp.bfloat16)[:, None, None, :, None] * placed[None, :, :, None, :]
    halves = halves.reshape(2 * width, peers * CAP * 2 * cells)

    far, near, across = lax.axis_size("z"), lax.axis_size(("y", "c")), lax.axis_size("x")
    sent = jax.ShapeDtypeStruct((near * across, far, observer_points.shape[1]), jnp.float32)
    parts = radiate(halves, arrived, panel_normals.T, table, made, sent)
    parts = jnp.sum(lax.all_to_all(parts, SLAB, 0, 0, tiled=True), axis=0)
    parts = lax.all_to_all(parts.reshape(far, 1, -1), "z", 0, 0, tiled=True)
    return jnp.sum(parts, axis=0)


def solution(mesh):
    panel, obs = mesh.shape["panel"], mesh.shape["obs"]
    finer = Mesh(mesh.devices.reshape(panel // 8, 4, 2, obs), ("z", "y", "c", "x"))
    every = PANEL + ("x",)
    in_specs = (
        P(PANEL, None, None),
        P(every, None, None),
        P(every, None),
        P(every),
        P(None, every),
        P(None, every),
        P(None, "x"),
    )
    return jax.shard_map(body, mesh=finer, in_specs=in_specs, out_specs=P(PANEL, "x"), check_vma=False)
```

```python
import functools
import math

import jax
import jax.numpy as jnp
from jax import lax
from jax.experimental import pallas as pl
from jax.experimental.pallas import tpu as pltpu
from jax.sharding import Mesh
from jax.sharding import PartitionSpec as P

NV = 5
NT = 256
HARM = 64
KAPPA = 0.5
PANEL = ("z", "y", "c")
CAP = 2
GROUP = 8
PANEL_STEP = 32
TOGETHER = 4
OBS_TILE = 256


def harmonic_of(index):
    return (index % GROUP) * (HARM // GROUP) + index // GROUP + 1


def fourier_table(samples, orders):
    sample_ids = jnp.arange(samples, dtype=jnp.int32)
    harmonic = harmonic_of(jnp.arange(orders, dtype=jnp.int32))
    wrapped = sample_ids[:, None] * harmonic[None, :] % samples
    angles = wrapped.astype(jnp.float32) * (2.0 * math.pi / samples)
    factor = 2.0 / samples
    return jnp.concatenate([factor * jnp.cos(angles), -factor * jnp.sin(angles)], axis=1)


def geometry_kernel(points_ref, observers_ref, made_ref):
    basis_ref, cos_ref, sin_ref = (made_ref.at[n] for n in range(3))
    panels = points_ref.shape[0]
    offsets = [observers_ref[i : i + 1, :] - points_ref[:, i : i + 1] for i in range(3)]
    distance = jnp.sqrt(offsets[0] * offsets[0] + offsets[1] * offsets[1] + offsets[2] * offsets[2])
    inverse = 1.0 / distance
    weight = inverse * (1.0 / (4.0 * math.pi))
    near = weight * inverse
    rows = lambda j: pl.ds(j, panels, stride=GROUP)
    for i in range(3):
        direction = offsets[i] * inverse
        basis_ref[rows(i), :] = direction * near
        basis_ref[rows(3 + i), :] = direction * weight
    basis_ref[rows(6), :] = weight
    basis_ref[rows(7), :] = jnp.zeros_like(weight)
    phase = KAPPA * distance
    c, s = jnp.cos(phase), jnp.sin(phase)
    c8, s8 = c, s
    for _ in range(3):
        c8, s8 = c8 * c8 - s8 * s8, 2.0 * (s8 * c8)
    for j in range(GROUP):
        cos_ref[rows(j), :] = c
        sin_ref[rows(j), :] = s
        c, s = c * c8 - s * s8, s * c8 + c * s8


def geometry(points, observers):
    panels, total = points.shape[0], observers.shape[1]
    tile = 128
    return pl.pallas_call(
        geometry_kernel,
        grid=(total // tile,),
        out_shape=jax.ShapeDtypeStruct((3, panels * GROUP, total), jnp.float32),
        in_specs=[
            pl.BlockSpec((panels, 3), lambda x: (0, 0)),
            pl.BlockSpec((3, tile), lambda x: (0, x)),
        ],
        out_specs=pl.BlockSpec((3, panels * GROUP, tile), lambda x: (0, 0, x)),
        cost_estimate=pl.CostEstimate(
            flops=200 * panels * total, bytes_accessed=12 * panels * GROUP * total, transcendentals=3 * panels * total
        ),
        name="geometry",
    )(points, observers)


def split_two(value):
    high = value.astype(jnp.bfloat16).astype(jnp.float32)
    return high, value - high


def fill_factors(weights_ref, donors_ref, normals_ref, table_ref, factors_ref):
    slots, pairs, rows8, lanes128 = donors_ref.shape
    panels = normals_ref.shape[0]
    columns = []
    for t in range(pairs):
        block = donors_ref[:, t].reshape(slots * rows8, lanes128)
        both = jnp.dot(weights_ref[...], block, preferred_element_type=jnp.float32)
        columns += [both[:panels], both[panels:]]
    per = NT // lanes128
    field = lambda v: jnp.concatenate(columns[v * per : (v + 1) * per], axis=1)
    normal = [normals_ref[:, i : i + 1] for i in range(3)]
    flow = field(1) * normal[0] + field(2) * normal[1] + field(3) * normal[2]
    mass = (1.0 + field(0)) * flow
    loads = [field(4) * normal[i] + mass * field(1 + i) for i in range(3)]
    series = jnp.concatenate([mass] + loads, axis=0)
    spectra = jnp.dot(series, table_ref[...], precision=lax.Precision.HIGHEST, preferred_element_type=jnp.float32)
    lane = lax.broadcasted_iota(jnp.int32, (panels, 2 * HARM), 1)
    order = harmonic_of(jnp.where(lane < HARM, lane, lane - HARM)).astype(jnp.float32) * KAPPA
    wave = jnp.where(lane < HARM, -order, order)
    rows = lambda j: pl.ds(j, panels, stride=GROUP)
    for i in range(4):
        part = spectra[i * panels : (i + 1) * panels]
        turned = jnp.concatenate([part[:, HARM:], part[:, :HARM]], axis=1) * wave
        if i == 0:
            factors_ref[rows(6), :] = turned
        else:
            factors_ref[rows(i - 1), :] = part
            factors_ref[rows(2 + i), :] = turned
    factors_ref[rows(7), :] = jnp.zeros((panels, 2 * HARM), jnp.float32)


def left_factors(first, factors_ref):
    lefts = []
    for k in range(TOGETHER):
        high, low = split_two(factors_ref[pl.ds(pl.multiple_of((first + k) * GROUP, GROUP), GROUP), :])
        lefts.append(jnp.concatenate([high, high, low, jnp.zeros_like(low)], axis=0).astype(jnp.bfloat16))
    return lefts


def amplitudes(first, lefts, lanes, basis_ref, amps_ref):
    for k in range(TOGETHER):
        at = pl.multiple_of((first + k) * GROUP, GROUP)
        high, low = split_two(basis_ref[pl.ds(at, GROUP), lanes])
        right = jnp.concatenate([high, low, high, jnp.zeros_like(low)], axis=0).astype(jnp.bfloat16)
        amps_ref[k, :, lanes] = lax.dot_general(
            lefts[k], right, (((0,), (0,)), ((), ())), preferred_element_type=jnp.float32
        )


def add_up(first, lanes, amps_ref, cos_ref, sin_ref, sent_ref):
    width = sent_ref.shape[2]
    block, inner = lanes.start // width, slice(lanes.start % width, lanes.start % width + 128)
    across = cos_ref.shape[1] // width
    cores = sent_ref.shape[0] // across
    states = []
    for k in range(TOGETHER):
        at = pl.multiple_of((first + k) * GROUP, GROUP)
        c, s = cos_ref[pl.ds(at, GROUP), lanes], sin_ref[pl.ds(at, GROUP), lanes]
        c1 = jnp.broadcast_to(c[0:1, :], c.shape)
        s1 = jnp.broadcast_to(s[0:1, :], s.shape)
        states.append((c, s, c * c1 + s * s1, s * c1 - c * s1, 2.0 * c1))
    for r in range(HARM // GROUP):
        re = slice(r * GROUP, (r + 1) * GROUP)
        im = slice(HARM + r * GROUP, HARM + (r + 1) * GROUP)
        y, c_core = r // cores, r % cores
        place = c_core * across + block
        low = slice(2 * GROUP * y, 2 * GROUP * y + GROUP)
        high = slice(2 * GROUP * y + GROUP, 2 * GROUP * (y + 1))
        total_re, total_im = sent_ref[place, low, inner], sent_ref[place, high, inner]
        for k in range(TOGETHER):
            c, s, before_c, before_s, twice = states[k]
            a_re, a_im = amps_ref[k, re, lanes], amps_ref[k, im, lanes]
            total_re = total_re + (a_re * c + a_im * s)
            total_im = total_im + (a_im * c - a_re * s)
            states[k] = (twice * c - before_c, twice * s - before_s, c, s, twice)
        sent_ref[place, low, inner] = total_re
        sent_ref[place, high, inner] = total_im


def radiate_kernel(
    weights_ref,
    donors_ref,
    normals_ref,
    table_ref,
    made_hbm,
    sent_ref,
    made_ref,
    factors_ref,
    even_ref,
    odd_ref,
    arrived,
):
    size = PANEL_STEP * GROUP
    basis_ref, cos_ref, sin_ref = (made_ref.at[n] for n in range(3))

    def fetch(chunk):
        rows = pl.ds(pl.multiple_of(chunk * size, size), size)
        return pltpu.make_async_copy(made_hbm.at[:, rows, :], made_ref.at[:, rows, :], arrived.at[chunk])

    panels = normals_ref.shape[0]
    for chunk in range(panels // PANEL_STEP):
        fetch(chunk).start()
    fill_factors(weights_ref, donors_ref, normals_ref, table_ref, factors_ref)
    sent_ref[...] = jnp.zeros_like(sent_ref)
    fetch(0).wait()

    last = panels - TOGETHER
    observers = basis_ref.shape[1]
    tiles = [slice(x, x + OBS_TILE) for x in range(0, observers, OBS_TILE)]
    parts = [slice(x, x + 128) for x in range(0, observers, 128)]

    lefts = left_factors(0, factors_ref)
    for lanes in tiles:
        amplitudes(0, lefts, lanes, basis_ref, even_ref)

    def one_group(turn, carry):
        first = turn * TOGETHER
        following = jnp.minimum(first + TOGETHER, last)
        due = (first + TOGETHER) // PANEL_STEP

        @pl.when(((first + TOGETHER) % PANEL_STEP == 0) & (first < last))
        def _():
            fetch(due).wait()

        def compute(now_ref, next_ref):
            lefts = left_factors(following, factors_ref)
            share = len(parts) // (len(tiles) + 1)
            done = 0
            for lanes in tiles:
                for part in parts[done : done + share]:
                    add_up(first, part, now_ref, cos_ref, sin_ref, sent_ref)
                done += share
                amplitudes(following, lefts, lanes, basis_ref, next_ref)
            for part in parts[done:]:
                add_up(first, part, now_ref, cos_ref, sin_ref, sent_ref)

        pl.when(turn % 2 == 0)(lambda: compute(even_ref, odd_ref))
        pl.when(turn % 2 == 1)(lambda: compute(odd_ref, even_ref))
        return carry

    lax.fori_loop(0, panels // TOGETHER, one_group, 0)


def radiate(weights, donors, normals, table, made, sent):
    panels, observers = normals.shape[0], made.shape[2]
    near, far = pl.BlockSpec(memory_space=pltpu.VMEM), pl.BlockSpec(memory_space=pltpu.HBM)
    amps = pltpu.VMEM((TOGETHER, 2 * HARM, observers), jnp.float32)
    return pl.pallas_call(
        radiate_kernel,
        out_shape=sent,
        in_specs=[near, near, near, near, far],
        out_specs=near,
        scratch_shapes=[
            pltpu.VMEM(made.shape, jnp.float32),
            pltpu.VMEM((panels * GROUP, 2 * HARM), jnp.float32),
            amps,
            amps,
            pltpu.SemaphoreType.DMA((panels // PANEL_STEP,)),
        ],
        compiler_params=pltpu.CompilerParams(
            vmem_limit_bytes=46 * 2**20
        ),
        cost_estimate=pl.CostEstimate(
            flops=30 * panels * HARM * observers, bytes_accessed=12 * panels * GROUP * observers, transcendentals=0
        ),
        name="radiate",
    )(weights, donors, normals, table, made)


def gather_kernel(asked_ref, blocks_ref, found_ref, sent):
    peers = found_ref.shape[0]

    def one_peer(peer, carry):
        word = asked_ref[peer, 0, 0]
        pltpu.make_async_copy(blocks_ref.at[word & 0xFFFF], found_ref.at[peer, 0], sent).start()
        pltpu.make_async_copy(blocks_ref.at[word >> 16], found_ref.at[peer, 1], sent).start()
        return carry

    lax.fori_loop(0, peers, one_peer, 0, unroll=8)
    pltpu.make_async_copy(found_ref, found_ref, sent).wait()


def gather(asked, blocks):
    return pl.pallas_call(
        gather_kernel,
        in_specs=[pl.BlockSpec(memory_space=pltpu.SMEM), pl.BlockSpec(memory_space=pltpu.VMEM)],
        out_specs=pl.BlockSpec(memory_space=pltpu.HBM),
        out_shape=jax.ShapeDtypeStruct((asked.shape[0], CAP) + blocks.shape[1:], blocks.dtype),
        scratch_shapes=[pltpu.SemaphoreType.DMA],
        name="gather",
    )(asked, blocks)


def body(flow_blocks, interp_weights, donor_owner, donor_block, panel_normals, panel_points, observer_points):
    peers = lax.axis_size(PANEL)
    cells, history = flow_blocks.shape[1:]
    width = interp_weights.shape[1]
    slots = donor_block.shape[0]
    owner = donor_owner[:, 0]

    held = flow_blocks.shape[0]
    named = owner[:, None] == jnp.arange(peers, dtype=jnp.int32)[None, :]
    lower = jnp.min(jnp.where(named, donor_block[:, None], held), axis=0)
    higher = jnp.max(jnp.where(named, donor_block[:, None], 0), axis=0)
    requests = jnp.where(lower == held, 0, lower) + (higher << 16)
    requests = lax.optimization_barrier(requests)
    asked = lax.all_to_all(requests.reshape(peers, 1, 1), PANEL, 0, 0, tiled=True)
    tiles = history // 256
    blocks = flow_blocks.reshape(held, cells, tiles, 2, 128).transpose(0, 2, 3, 1, 4).reshape(held, tiles, 2 * cells, 128)
    arrived = lax.all_to_all(gather(asked, blocks), PANEL, 0, 0, tiled=True).reshape(peers * CAP, tiles, 2 * cells, 128)

    observer_points, owner, donor_block, _ = lax.optimization_barrier((observer_points, owner, donor_block, asked))
    observers = lax.all_gather(observer_points, "x", axis=1, tiled=True)
    made = geometry(panel_points.T, observers)
    table = fourier_table(NT, HARM)
    row = jnp.arange(slots, dtype=jnp.int32)
    key = donor_block * slots + row
    rank = jnp.sum(((owner[:, None] == owner[None, :]) & (key[None, :] < key[:, None])).astype(jnp.int32), axis=1)
    chosen = (owner * CAP + rank)[:, None] == jnp.arange(peers * CAP, dtype=jnp.int32)[None, :]
    placing = chosen.astype(jnp.bfloat16)
    weights = interp_weights.reshape(width, slots, cells)
    placed = jnp.einsum("prc,rs->psc", weights, placing, preferred_element_type=jnp.float32).astype(jnp.bfloat16)
    halves = jnp.eye(2, dtype=jnp.bfloat16)[:, None, None, :, None] * placed[None, :, :, None, :]
    halves = halves.reshape(2 * width, peers * CAP * 2 * cells)

    here, away = lax.axis_size(("c", "x")), lax.axis_size(("y", "z"))
    sent = jax.ShapeDtypeStruct((here, away, observer_points.shape[1]), jnp.float32)
    parts = radiate(halves, arrived, panel_normals.T, table, made, sent)
    parts = jnp.sum(lax.all_to_all(parts, ("c", "x"), 0, 0, tiled=True), axis=0)
    parts = lax.all_to_all(parts.reshape(away, 1, -1), ("y", "z"), 0, 0, tiled=True)
    return jnp.sum(parts, axis=0)


def solution(mesh):
    panel, obs = mesh.shape["panel"], mesh.shape["obs"]
    finer = Mesh(mesh.devices.reshape(panel // 8, 4, 2, obs), ("z", "y", "c", "x"))
    every = PANEL + ("x",)
    in_specs = (
        P(PANEL, None, None),
        P(every, None, None),
        P(every, None),
        P(every),
        P(None, every),
        P(None, every),
        P(None, "x"),
    )
    return jax.shard_map(body, mesh=finer, in_specs=in_specs, out_specs=P(PANEL, "x"), check_vma=False)
```

```python
import functools
import math

import jax
import jax.numpy as jnp
from jax import lax
from jax.experimental import pallas as pl
from jax.experimental.pallas import tpu as pltpu
from jax.sharding import Mesh
from jax.sharding import PartitionSpec as P

NV = 5
NT = 256
HARM = 64
KAPPA = 0.5
PANEL = ("z", "y", "c")
SLAB = ("y", "c", "x")
CAP = 2
GROUP = 8
PANEL_STEP = 32
TOGETHER = 4
OBS_TILE = 256


def harmonic_of(index):
    return (index % GROUP) * (HARM // GROUP) + index // GROUP + 1


def fourier_table(samples, orders):
    sample_ids = jnp.arange(samples, dtype=jnp.int32)
    harmonic = harmonic_of(jnp.arange(orders, dtype=jnp.int32))
    wrapped = sample_ids[:, None] * harmonic[None, :] % samples
    angles = wrapped.astype(jnp.float32) * (2.0 * math.pi / samples)
    factor = 2.0 / samples
    return jnp.concatenate([factor * jnp.cos(angles), -factor * jnp.sin(angles)], axis=1)


def geometry_kernel(points_ref, observers_ref, made_ref):
    basis_ref, cos_ref, sin_ref = (made_ref.at[n] for n in range(3))
    panels = points_ref.shape[0]
    offsets = [observers_ref[i : i + 1, :] - points_ref[:, i : i + 1] for i in range(3)]
    distance = jnp.sqrt(offsets[0] * offsets[0] + offsets[1] * offsets[1] + offsets[2] * offsets[2])
    inverse = 1.0 / distance
    weight = inverse * (1.0 / (4.0 * math.pi))
    near = weight * inverse
    rows = lambda j: pl.ds(j, panels, stride=GROUP)
    for i in range(3):
        direction = offsets[i] * inverse
        basis_ref[rows(i), :] = direction * near
        basis_ref[rows(3 + i), :] = direction * weight
    basis_ref[rows(6), :] = weight
    basis_ref[rows(7), :] = jnp.zeros_like(weight)
    phase = KAPPA * distance
    c, s = jnp.cos(phase), jnp.sin(phase)
    c8, s8 = c, s
    for _ in range(3):
        c8, s8 = c8 * c8 - s8 * s8, 2.0 * (s8 * c8)
    for j in range(GROUP):
        cos_ref[rows(j), :] = c
        sin_ref[rows(j), :] = s
        c, s = c * c8 - s * s8, s * c8 + c * s8


def geometry(points, observers):
    panels, total = points.shape[0], observers.shape[1]
    tile = 128
    return pl.pallas_call(
        geometry_kernel,
        grid=(total // tile,),
        out_shape=jax.ShapeDtypeStruct((3, panels * GROUP, total), jnp.float32),
        in_specs=[
            pl.BlockSpec((panels, 3), lambda x: (0, 0)),
            pl.BlockSpec((3, tile), lambda x: (0, x)),
        ],
        out_specs=pl.BlockSpec((3, panels * GROUP, tile), lambda x: (0, 0, x)),
        cost_estimate=pl.CostEstimate(
            flops=200 * panels * total, bytes_accessed=12 * panels * GROUP * total, transcendentals=3 * panels * total
        ),
        name="geometry",
    )(points, observers)


def split_two(value):
    high = value.astype(jnp.bfloat16).astype(jnp.float32)
    return high, value - high


def fill_factors(weights_ref, donors_ref, normals_ref, table_ref, factors_ref):
    slots, pairs, rows8, lanes128 = donors_ref.shape
    panels = normals_ref.shape[0]
    columns = []
    for t in range(pairs):
        block = donors_ref[:, t].reshape(slots * rows8, lanes128)
        both = jnp.dot(weights_ref[...], block, preferred_element_type=jnp.float32)
        columns += [both[:panels], both[panels:]]
    per = NT // lanes128
    field = lambda v: jnp.concatenate(columns[v * per : (v + 1) * per], axis=1)
    normal = [normals_ref[:, i : i + 1] for i in range(3)]
    flow = field(1) * normal[0] + field(2) * normal[1] + field(3) * normal[2]
    mass = (1.0 + field(0)) * flow
    loads = [field(4) * normal[i] + mass * field(1 + i) for i in range(3)]
    series = jnp.concatenate([mass] + loads, axis=0)
    spectra = jnp.dot(series, table_ref[...], precision=lax.Precision.HIGHEST, preferred_element_type=jnp.float32)
    lane = lax.broadcasted_iota(jnp.int32, (panels, 2 * HARM), 1)
    order = harmonic_of(jnp.where(lane < HARM, lane, lane - HARM)).astype(jnp.float32) * KAPPA
    wave = jnp.where(lane < HARM, -order, order)
    rows = lambda j: pl.ds(j, panels, stride=GROUP)
    for i in range(4):
        part = spectra[i * panels : (i + 1) * panels]
        turned = jnp.concatenate([part[:, HARM:], part[:, :HARM]], axis=1) * wave
        if i == 0:
            factors_ref[rows(6), :] = turned
        else:
            factors_ref[rows(i - 1), :] = part
            factors_ref[rows(2 + i), :] = turned
    factors_ref[rows(7), :] = jnp.zeros((panels, 2 * HARM), jnp.float32)


def left_factors(first, factors_ref):
    lefts = []
    for k in range(TOGETHER):
        high, low = split_two(factors_ref[pl.ds(pl.multiple_of((first + k) * GROUP, GROUP), GROUP), :])
        lefts.append(jnp.concatenate([high, high, low, jnp.zeros_like(low)], axis=0).astype(jnp.bfloat16))
    return lefts


def amplitudes(first, lefts, lanes, basis_ref, amps_ref):
    for k in range(TOGETHER):
        at = pl.multiple_of((first + k) * GROUP, GROUP)
        high, low = split_two(basis_ref[pl.ds(at, GROUP), lanes])
        right = jnp.concatenate([high, low, high, jnp.zeros_like(low)], axis=0).astype(jnp.bfloat16)
        amps_ref[k, :, lanes] = lax.dot_general(
            lefts[k], right, (((0,), (0,)), ((), ())), preferred_element_type=jnp.float32
        )


def add_up(first, lanes, amps_ref, cos_ref, sin_ref, sent_ref):
    width = sent_ref.shape[2]
    block, inner = lanes.start // width, slice(lanes.start % width, lanes.start % width + 128)
    across = cos_ref.shape[1] // width
    states = []
    for k in range(TOGETHER):
        at = pl.multiple_of((first + k) * GROUP, GROUP)
        c, s = cos_ref[pl.ds(at, GROUP), lanes], sin_ref[pl.ds(at, GROUP), lanes]
        c1 = jnp.broadcast_to(c[0:1, :], c.shape)
        s1 = jnp.broadcast_to(s[0:1, :], s.shape)
        states.append((c, s, c * c1 + s * s1, s * c1 - c * s1, 2.0 * c1))
    for r in range(HARM // GROUP):
        re = slice(r * GROUP, (r + 1) * GROUP)
        im = slice(HARM + r * GROUP, HARM + (r + 1) * GROUP)
        place = r * across + block
        total_re, total_im = sent_ref[place, 0:GROUP, inner], sent_ref[place, GROUP : 2 * GROUP, inner]
        for k in range(TOGETHER):
            c, s, before_c, before_s, twice = states[k]
            a_re, a_im = amps_ref[k, re, lanes], amps_ref[k, im, lanes]
            total_re = total_re + (a_re * c + a_im * s)
            total_im = total_im + (a_im * c - a_re * s)
            states[k] = (twice * c - before_c, twice * s - before_s, c, s, twice)
        sent_ref[place, 0:GROUP, inner] = total_re
        sent_ref[place, GROUP : 2 * GROUP, inner] = total_im


def radiate_kernel(
    weights_hbm,
    donors_ref,
    normals_ref,
    table_ref,
    made_hbm,
    sent_ref,
    made_ref,
    factors_ref,
    even_ref,
    odd_ref,
    weights_ref,
    arrived,
    weighed,
):
    size = PANEL_STEP * GROUP
    basis_ref, cos_ref, sin_ref = (made_ref.at[n] for n in range(3))

    def fetch(chunk):
        rows = pl.ds(pl.multiple_of(chunk * size, size), size)
        return pltpu.make_async_copy(made_hbm.at[:, rows, :], made_ref.at[:, rows, :], arrived.at[chunk])

    panels = normals_ref.shape[0]
    weigh = pltpu.make_async_copy(weights_hbm, weights_ref, weighed)
    weigh.start()
    for chunk in range(panels // PANEL_STEP):
        fetch(chunk).start()
    sent_ref[...] = jnp.zeros_like(sent_ref)
    weigh.wait()
    fill_factors(weights_ref, donors_ref, normals_ref, table_ref, factors_ref)
    fetch(0).wait()

    last = panels - TOGETHER
    observers = basis_ref.shape[1]
    tiles = [slice(x, x + OBS_TILE) for x in range(0, observers, OBS_TILE)]
    parts = [slice(x, x + 128) for x in range(0, observers, 128)]

    lefts = left_factors(0, factors_ref)
    for lanes in tiles:
        amplitudes(0, lefts, lanes, basis_ref, even_ref)

    def one_group(turn, carry):
        first = turn * TOGETHER
        following = jnp.minimum(first + TOGETHER, last)
        due = (first + TOGETHER) // PANEL_STEP

        @pl.when(((first + TOGETHER) % PANEL_STEP == 0) & (first < last))
        def _():
            fetch(due).wait()

        def compute(now_ref, next_ref):
            lefts = left_factors(following, factors_ref)
            share = len(parts) // (len(tiles) + 1)
            done = 0
            for lanes in tiles:
                for part in parts[done : done + share]:
                    add_up(first, part, now_ref, cos_ref, sin_ref, sent_ref)
                done += share
                amplitudes(following, lefts, lanes, basis_ref, next_ref)
            for part in parts[done:]:
                add_up(first, part, now_ref, cos_ref, sin_ref, sent_ref)

        pl.when(turn % 2 == 0)(lambda: compute(even_ref, odd_ref))
        pl.when(turn % 2 == 1)(lambda: compute(odd_ref, even_ref))
        return carry

    lax.fori_loop(0, panels // TOGETHER, one_group, 0)


def radiate(weights, donors, normals, table, made, sent):
    panels, observers = normals.shape[0], made.shape[2]
    near, far = pl.BlockSpec(memory_space=pltpu.VMEM), pl.BlockSpec(memory_space=pltpu.HBM)
    amps = pltpu.VMEM((TOGETHER, 2 * HARM, observers), jnp.float32)
    return pl.pallas_call(
        radiate_kernel,
        out_shape=sent,
        in_specs=[far, near, near, near, far],
        out_specs=near,
        scratch_shapes=[
            pltpu.VMEM(made.shape, jnp.float32),
            pltpu.VMEM((panels * GROUP, 2 * HARM), jnp.float32),
            amps,
            amps,
            pltpu.VMEM(weights.shape, weights.dtype),
            pltpu.SemaphoreType.DMA((panels // PANEL_STEP,)),
            pltpu.SemaphoreType.DMA,
        ],
        compiler_params=pltpu.CompilerParams(
            vmem_limit_bytes=46 * 2**20
        ),
        cost_estimate=pl.CostEstimate(
            flops=30 * panels * HARM * observers, bytes_accessed=12 * panels * GROUP * observers, transcendentals=0
        ),
        name="radiate",
    )(weights, donors, normals, table, made)


def gather_kernel(asked_ref, blocks_ref, found_ref, sent):
    peers = found_ref.shape[0]

    def one_peer(peer, carry):
        word = asked_ref[peer, 0, 0]
        pltpu.make_async_copy(blocks_ref.at[word & 0xFFFF], found_ref.at[peer, 0], sent).start()
        pltpu.make_async_copy(blocks_ref.at[word >> 16], found_ref.at[peer, 1], sent).start()
        return carry

    lax.fori_loop(0, peers, one_peer, 0, unroll=8)
    pltpu.make_async_copy(found_ref, found_ref, sent).wait()


def gather(asked, blocks):
    return pl.pallas_call(
        gather_kernel,
        in_specs=[pl.BlockSpec(memory_space=pltpu.SMEM), pl.BlockSpec(memory_space=pltpu.VMEM)],
        out_specs=pl.BlockSpec(memory_space=pltpu.HBM),
        out_shape=jax.ShapeDtypeStruct((asked.shape[0], CAP) + blocks.shape[1:], blocks.dtype),
        scratch_shapes=[pltpu.SemaphoreType.DMA],
        name="gather",
    )(asked, blocks)


def body(flow_blocks, interp_weights, donor_owner, donor_block, panel_normals, panel_points, observer_points):
    peers = lax.axis_size(PANEL)
    cells, history = flow_blocks.shape[1:]
    width = interp_weights.shape[1]
    slots = donor_block.shape[0]
    owner = donor_owner[:, 0]

    held = flow_blocks.shape[0]
    named = owner[:, None] == jnp.arange(peers, dtype=jnp.int32)[None, :]
    lower = jnp.min(jnp.where(named, donor_block[:, None], held), axis=0)
    higher = jnp.max(jnp.where(named, donor_block[:, None], 0), axis=0)
    requests = jnp.where(lower == held, 0, lower) + (higher << 16)
    requests = lax.optimization_barrier(requests)
    asked = lax.all_to_all(requests.reshape(peers, 1, 1), PANEL, 0, 0, tiled=True)
    tiles = history // 256
    blocks = flow_blocks.reshape(held, cells, tiles, 2, 128).transpose(0, 2, 3, 1, 4).reshape(held, tiles, 2 * cells, 128)
    arrived = lax.all_to_all(gather(asked, blocks), PANEL, 0, 0, tiled=True).reshape(peers * CAP, tiles, 2 * cells, 128)

    observer_points, owner, donor_block, _ = lax.optimization_barrier((observer_points, owner, donor_block, asked))
    observers = lax.all_gather(observer_points, "x", axis=1, tiled=True)
    made = geometry(panel_points.T, observers)
    table = fourier_table(NT, HARM)
    row = jnp.arange(slots, dtype=jnp.int32)
    key = donor_block * slots + row
    rank = jnp.sum(((owner[:, None] == owner[None, :]) & (key[None, :] < key[:, None])).astype(jnp.int32), axis=1)
    chosen = (owner * CAP + rank)[:, None] == jnp.arange(peers * CAP, dtype=jnp.int32)[None, :]
    placing = chosen.astype(jnp.bfloat16)
    weights = interp_weights.reshape(width, slots, cells)
    placed = jnp.einsum("prc,rs->psc", weights, placing, preferred_element_type=jnp.float32).astype(jnp.bfloat16)
    halves = jnp.eye(2, dtype=jnp.bfloat16)[:, None, None, :, None] * placed[None, :, :, None, :]
    halves = halves.reshape(2 * width, peers * CAP * 2 * cells)

    far, near, across = lax.axis_size("z"), lax.axis_size(("y", "c")), lax.axis_size("x")
    sent = jax.ShapeDtypeStruct((near * across, far, observer_points.shape[1]), jnp.float32)
    parts = radiate(halves, arrived, panel_normals.T, table, made, sent)
    parts = jnp.sum(lax.all_to_all(parts, SLAB, 0, 0, tiled=True), axis=0)
    parts = lax.all_to_all(parts.reshape(far, 1, -1), "z", 0, 0, tiled=True)
    return jnp.sum(parts, axis=0)


def solution(mesh):
    panel, obs = mesh.shape["panel"], mesh.shape["obs"]
    finer = Mesh(mesh.devices.reshape(panel // 8, 4, 2, obs), ("z", "y", "c", "x"))
    every = PANEL + ("x",)
    in_specs = (
        P(PANEL, None, None),
        P(every, None, None),
        P(every, None),
        P(every),
        P(None, every),
        P(None, every),
        P(None, "x"),
    )
    return jax.shard_map(body, mesh=finer, in_specs=in_specs, out_specs=P(PANEL, "x"), check_vma=False)
```
